32 devices in a mesh: seg: 8 (over z, x), mp: 4 (over y, core).
Axes of the slice: x: 2, y: 2, z: 4, core: 2. Of those that a mesh axis runs over, the one named last changes fastest.
Arguments:
- embedded: bfloat16 [4096, 1024], P('seg'), may hold values from -6 to 6
- targets: int32 [4096], P('seg'), may hold values from 0 to 10239
- pred_device: int32 [8], P('seg'), may hold values from -1 to 7, as said below
- doc_ids: int32 [8], P('seg'), may hold values from 0 to 1, as said below
- valid_rows: int32 [8], P('seg'), may hold values from 1 to 512, as said below
- w_query: bfloat16 [1024, 1024], P(None, 'mp'), may hold values from -8 to 8
- w_key: bfloat16 [1024, 1024], P(None, 'mp'), may hold values from -1 to 1
- w_value: bfloat16 [1024, 1024], P(None, 'mp'), may hold values from -0.1875 to 0.1875
- w_rel: bfloat16 [1024, 1024], P(None, 'mp'), may hold values from -0.1875 to 0.1875
- content_bias: float32 [16, 64], P('mp'), may hold values from -3 to 3
- position_bias: float32 [16, 64], P('mp'), may hold values from -8 to 8
- attn_out: bfloat16 [1024, 1024], P('mp'), may hold values from -0.1875 to 0.1875
- attn_gain: float32 [1024], replicated, may hold values from 0.25 to 1.75
- attn_shift: float32 [1024], replicated, may hold values from -3 to 3
- w_up: bfloat16 [1024, 4096], P(None, 'mp'), may hold values from -0.1875 to 0.1875
- up_bias: float32 [4096], P('mp'), may hold values from -3 to 3
- w_down: bfloat16 [4096, 1024], P('mp'), may hold values from -0.09375 to 0.09375
- down_bias: float32 [1024], replicated, may hold values from -3 to 3
- ffn_gain: float32 [1024], replicated, may hold values from 0.25 to 1.75
- ffn_shift: float32 [1024], replicated, may hold values from -3 to 3
- w_vocab: bfloat16 [1024, 10240], P(None, 'mp'), may hold values from -8 to 8
Outputs:
- token_loglik: float32 [4096], P('seg')
- doc_loglik: float32 [2], replicated
The draws below stay inside these ranges and needn't reach their ends.
Inputs may be any that keep to these rules, and one draw needn't show every extreme that they name: `pred_device`: -1 for the first segment of a document, else the device of the document's previous segment, which lies from 3 devices below to 1 devices above; no device is named by two devices. `doc_ids`: every document holds one or more whole segments, chained by pred_device. `valid_rows`: 512 except on the last segment of a document.
All inputs are finite; a program needn't handle non-finite values.
Results may differ from the reference program's by a relative error of at most 0.007.
Values may be sent and summed in bfloat16 or wider, within the bound.
No kernel may reach another device: no remote copies, remote signals or barrier semaphores. Data moves between devices by JAX's collectives and lax.ppermute only.
A program may use at most 128 MiB of HBM per device.

```python
import math
import jax
import jax.numpy as jnp
import numpy as np
from jax import lax

D = 1024
H = 16
DH = 64
FF = 4096
VOCAB = 10240
SEG = 512
SPREAD = 2
TOKENS = 4096
DOCS = 2
N_SEG = 8
N_MP = 4


def layout(key):
    base_key = jax.random.fold_in(key, 4301)
    cut_key = jax.random.fold_in(base_key, 1)
    order_key = jax.random.fold_in(base_key, 2)
    fill_key = jax.random.fold_in(base_key, 3)
    cut_points = jax.random.permutation(cut_key, N_SEG - 1)[:DOCS - 1] + 1
    starts = jnp.zeros((N_SEG,), jnp.int32).at[0].set(1).at[cut_points].set(1)
    doc_order = jnp.cumsum(starts) - 1
    block_keys = jax.random.split(order_key, N_SEG // SPREAD)
    shuffle = jax.vmap(lambda block_key: jax.random.permutation(block_key, SPREAD))(block_keys)
    placed = jnp.arange(N_SEG) // SPREAD * SPREAD + shuffle.reshape(-1)
    placed = placed.astype(jnp.int32)
    before = jnp.concatenate([jnp.full((1,), -1, jnp.int32), placed[:-1]])
    pred_order = jnp.where(starts == 1, -1, before)
    closing = jnp.concatenate([starts[1:], jnp.ones((1,), jnp.int32)])
    fill_rows = jax.random.randint(fill_key, (N_SEG,), 1, SEG + 1)
    valid_order = jnp.where(closing == 1, fill_rows, SEG)
    pred_device = jnp.zeros((N_SEG,), jnp.int32).at[placed].set(pred_order)
    doc_ids = jnp.zeros((N_SEG,), jnp.int32).at[placed].set(doc_order.astype(jnp.int32))
    valid_rows = jnp.zeros((N_SEG,), jnp.int32).at[placed].set(valid_order.astype(jnp.int32))
    return (pred_device, doc_ids, valid_rows)


def draw_pred_device(key, part):
    return layout(key)[0]


def draw_doc_ids(key, part):
    return layout(key)[1]


def draw_valid_rows(key, part):
    return layout(key)[2]


def projection_pair(key):
    shape_qk = (D, H * DH)
    key_base = jax.random.fold_in(key, 4101)
    query_base = jax.random.fold_in(key, 4102)
    key_part = jnp.clip(jax.random.normal(key_base, shape_qk, jnp.float32), -6.0, 6.0) * D ** (-0.5)
    query_part = jnp.clip(jax.random.normal(query_base, shape_qk, jnp.float32), -6.0, 6.0) * D ** (-0.5)
    return (query_part, key_part)


def draw_w_query(key, part):
    return projection_pair(key)[0].astype(jnp.bfloat16)


def draw_w_key(key, part):
    return projection_pair(key)[1].astype(jnp.bfloat16)


def draw_w_vocab(key, part):
    shape_out = (D, VOCAB)
    entry_key = jax.random.fold_in(key, 4201)
    return (jnp.clip(jax.random.normal(entry_key, shape_out, jnp.float32), -6.0, 6.0) * 0.1).astype(jnp.bfloat16)


def place_ends(array, rng, least, top_value):
    shape = array.shape
    spot = [jax.random.randint(jax.random.fold_in(rng, axis), (), 0, shape[axis]) for axis in range(len(shape))]
    array = array.at[tuple(spot)].set(least)
    longest = shape.index(max(shape))
    spot[longest] = (spot[longest] + 1) % shape[longest]
    return array.at[tuple(spot)].set(top_value)


def block_scale(key, dims, cuts, smallest, high):
    loudness, own = 1.0, jax.random.fold_in(key, 6)
    for axis_at, shards_of in cuts:
        heights = jnp.exp(jax.random.uniform(jax.random.fold_in(own, axis_at), (shards_of,), jnp.float32, smallest / len(cuts), high / len(cuts)))
        loudness = loudness * jnp.repeat(heights, dims[axis_at] // shards_of).reshape([-1 if axis == axis_at else 1 for axis in range(len(dims))])
    return loudness


def rank_table(amount, slope):
    loads = [(1 << 20) // math.isqrt(standing ** slope) + 1 for standing in range(1, amount + 1)]
    scale = 1 + sum(loads) // (1 << 30)
    return np.cumsum(np.array([max(1, weight // scale) for weight in loads]))


def ranked(stream_key, dims, number_of, lean):
    table = rank_table(number_of, lean)
    lot = jax.random.randint(jax.random.fold_in(stream_key, 1), dims, 0, int(table[number_of - 1]))
    standing = jnp.searchsorted(jnp.asarray(table, jnp.int32), lot, side="right")
    return jax.random.permutation(jax.random.fold_in(stream_key, 2), number_of)[standing].astype(jnp.int32)


def noise(key, extent, scale, bound, cuts=(), dtype=jnp.bfloat16):
    loudness = block_scale(key, extent, cuts, -0.22, 0.18) if cuts else 1.0
    result = jax.random.normal(key, extent, jnp.float32) * scale * loudness
    return jnp.minimum(jnp.maximum(result, -bound), bound).astype(dtype)


def setup_inputs(seed: int = 0) -> dict:
    streams_of = jax.random.split(jax.random.key(seed), 22)
    return {
        "embedded": noise(streams_of[0], (TOKENS, D), 1.0, 6.0, ((0, 8),)),
        "targets": place_ends(ranked(streams_of[1], (TOKENS,), VOCAB, 2), jax.random.fold_in(streams_of[1], 3), 0, VOCAB - 1).astype(jnp.int32),
        "pred_device": draw_pred_device(jax.random.fold_in(streams_of[21], 71), 0),
        "doc_ids": draw_doc_ids(jax.random.fold_in(streams_of[21], 71), 0),
        "valid_rows": draw_valid_rows(jax.random.fold_in(streams_of[21], 71), 0),
        "w_query": draw_w_query(jax.random.fold_in(streams_of[21], 71), 0),
        "w_key": draw_w_key(jax.random.fold_in(streams_of[21], 71), 0),
        "w_value": noise(streams_of[7], (D, H * DH), D ** -0.5, 0.1875, ((1, 4),)),
        "w_rel": noise(streams_of[8], (D, H * DH), D ** -0.5, 0.1875, ((1, 4),)),
        "content_bias": noise(streams_of[9], (H, DH), 0.5, 3.0, ((0, 4),), jnp.float32),
        "position_bias": noise(streams_of[10], (H, DH), 2.0, 8.0, ((0, 4),), jnp.float32),
        "attn_out": noise(streams_of[11], (H * DH, D), (H * DH) ** -0.5, 0.1875, ((0, 4),)),
        "attn_gain": jnp.clip(1.0 + 0.15 * jax.random.normal(streams_of[12], (D,), jnp.float32), 0.25, 1.75),
        "attn_shift": noise(streams_of[13], (D,), 0.5, 3.0, (), jnp.float32),
        "w_up": noise(streams_of[14], (D, FF), D ** -0.5, 0.1875, ((1, 4),)),
        "up_bias": noise(streams_of[15], (FF,), 0.5, 3.0, ((0, 4),), jnp.float32),
        "w_down": noise(streams_of[16], (FF, D), FF ** -0.5, 0.09375, ((0, 4),)),
        "down_bias": noise(streams_of[17], (D,), 0.5, 3.0, (), jnp.float32),
        "ffn_gain": jnp.clip(1.0 + 0.15 * jax.random.normal(streams_of[18], (D,), jnp.float32), 0.25, 1.75),
        "ffn_shift": noise(streams_of[19], (D,), 0.5, 3.0, (), jnp.float32),
        "w_vocab": draw_w_vocab(jax.random.fold_in(streams_of[21], 71), 0),
    }


EPSILON = 1e-05

def rounded(values):
    return lax.optimization_barrier(values.astype(jnp.bfloat16)).astype(jnp.float32)

def normalize(values, norm_gain, norm_shift):
    centre = values - lax.optimization_barrier(jnp.mean(values, axis=-1, keepdims=True))
    spread = lax.optimization_barrier(jnp.mean(centre * centre, axis=-1, keepdims=True))
    return centre * lax.rsqrt(spread + EPSILON) * norm_gain + norm_shift

def position_table(length, features):
    places = jnp.arange(length).astype(jnp.float32)
    frequency = 10000.0 ** (-jnp.arange(0, features, 2).astype(jnp.float32) / features)
    angles = places[:, None] * frequency[None, :]
    return jnp.concatenate([jnp.sin(angles), jnp.cos(angles)], axis=1).astype(jnp.bfloat16)

def group_sum(operand, matrix):
    rows_n = operand.shape[0]
    pieces = operand.reshape(rows_n, N_MP, -1).astype(jnp.float32)
    blocks = matrix.reshape(N_MP, -1, matrix.shape[1]).astype(jnp.float32)
    partial_terms = jnp.einsum('rgk,gkd->grd', pieces, blocks)
    return lax.optimization_barrier(jnp.sum(rounded(partial_terms), axis=0))

def reference(embedded, targets, pred_device, doc_ids, valid_rows, w_query, w_key, w_value, w_rel, content_bias, position_bias, attn_out, attn_gain, attn_shift, w_up, up_bias, w_down, down_bias, ffn_gain, ffn_shift, w_vocab):
    head_count = content_bias.shape[0]
    head_dim = content_bias.shape[1]
    key_span = 2 * SEG
    score_scale = head_dim ** (-0.5)
    rel_keys = jnp.dot(position_table(key_span, D), w_rel, preferred_element_type=jnp.float32)
    rel_keys = rounded(rel_keys).reshape(key_span, head_count, head_dim)
    segments = embedded.reshape(N_SEG, SEG, D)
    memories = segments[jnp.maximum(pred_device, 0)]
    row_index = jnp.arange(SEG)[:, None]
    key_index = jnp.arange(key_span)[None, :]
    distance = row_index + SEG - key_index
    gather_index = jnp.clip(distance, 0, key_span - 1).astype(jnp.int32)
    causal = distance >= 0

    def one_segment(segment_items):
        current, memory, has_memory, target_rows, used_rows = segment_items
        keys_in = jnp.concatenate([memory, current], axis=0)
        queries = jnp.dot(current, w_query, preferred_element_type=jnp.float32)
        with_content = rounded(queries + content_bias.reshape(-1)).reshape(SEG, head_count, head_dim)
        with_position = rounded(queries + position_bias.reshape(-1)).reshape(SEG, head_count, head_dim)
        key_rows = rounded(jnp.dot(keys_in, w_key, preferred_element_type=jnp.float32)).reshape(key_span, head_count, head_dim)
        value_rows = rounded(jnp.dot(keys_in, w_value, preferred_element_type=jnp.float32)).reshape(key_span, head_count, head_dim)
        content_score = jnp.einsum('ihd,jhd->hij', with_content, key_rows)
        position_all = jnp.einsum('ihd,rhd->hir', with_position, rel_keys)
        position_score = jnp.take_along_axis(position_all, jnp.broadcast_to(gather_index[None], position_all.shape), axis=2)
        allowed = causal & ((key_index >= SEG) | has_memory)
        scores = jnp.where(allowed[None], (content_score + position_score) * score_scale, -1e+30)
        row_top = lax.optimization_barrier(jnp.max(scores, axis=-1, keepdims=True))
        exponent = jnp.where(allowed[None], jnp.exp(scores - row_top), 0.0)
        row_total = lax.optimization_barrier(jnp.sum(exponent, axis=-1, keepdims=True))
        weights = rounded(exponent / row_total)
        attended = jnp.einsum('hij,jhd->ihd', weights, value_rows).astype(jnp.bfloat16).reshape(SEG, head_count * head_dim)
        attended_sum = group_sum(attended, attn_out)
        first_out = normalize(current.astype(jnp.float32) + attended_sum, attn_gain, attn_shift).astype(jnp.bfloat16)
        units = jnp.maximum(jnp.dot(first_out, w_up, preferred_element_type=jnp.float32) + up_bias, 0.0).astype(jnp.bfloat16)
        ffn_out = group_sum(units, w_down)
        second = normalize(first_out.astype(jnp.float32) + ffn_out + down_bias, ffn_gain, ffn_shift).astype(jnp.bfloat16)
        logits = jnp.dot(second, w_vocab, preferred_element_type=jnp.float32)
        logit_top = lax.optimization_barrier(jnp.max(logits, axis=1))
        log_total = logit_top + jnp.log(lax.optimization_barrier(jnp.sum(jnp.exp(logits - logit_top[:, None]), axis=1)))
        picked = jnp.take_along_axis(logits, target_rows[:, None].astype(jnp.int32), axis=1)[:, 0]
        return jnp.where(jnp.arange(SEG) < used_rows, picked - log_total, 0.0)
    token_loglik = lax.map(one_segment, (segments, memories, pred_device >= 0, targets.reshape(N_SEG, SEG), valid_rows))
    doc_total = jax.ops.segment_sum(lax.optimization_barrier(jnp.sum(token_loglik, axis=1)), doc_ids, num_segments=DOCS)
    doc_rows = jax.ops.segment_sum(valid_rows.astype(jnp.float32), doc_ids, num_segments=DOCS)
    return (token_loglik.reshape(-1), doc_total / doc_rows)
```

```python
import jax
import jax.numpy as jnp
from jax import lax
from jax.experimental import pallas as pl
from jax.experimental.pallas import tpu as pltpu
from jax.sharding import PartitionSpec as P

DOC_SPAN = 4
EPSILON = 1e-05
STEP = 32
ROWS = 128
MASKED = -1e30
BF = jnp.bfloat16
F32 = jnp.float32


def swapped(block, axis, distance):
    return lax.ppermute(block, axis, [(i, i ^ distance) for i in range(lax.axis_size(axis))])


def dot(a, b):
    return jnp.dot(a, b, preferred_element_type=F32)


def dot_nt(a, b):
    return lax.dot_general(a, b, (((1,), (1,)), ((), ())), preferred_element_type=F32)


def full(shape):
    return pl.BlockSpec(shape, lambda *_: (0,) * len(shape))


def normalize(values, norm_gain, norm_shift):
    centre = values - jnp.mean(values, axis=-1, keepdims=True)
    spread = jnp.mean(centre * centre, axis=-1, keepdims=True)
    return centre * lax.rsqrt(spread + EPSILON) * norm_gain + norm_shift


def rel_kernel(coarse_ref, fine_ref, weight_ref, out_ref):
    half = coarse_ref.shape[2]
    group = 256 // STEP
    sin_fine = fine_ref[0][None]
    cos_fine = fine_ref[1][None]
    for block in range(coarse_ref.shape[1] // group):
        sin_coarse = coarse_ref[0, block * group : (block + 1) * group][:, None]
        cos_coarse = coarse_ref[1, block * group : (block + 1) * group][:, None]
        sines = (sin_coarse * cos_fine + cos_coarse * sin_fine).reshape(256, half).astype(BF)
        cosines = (cos_coarse * cos_fine - sin_coarse * sin_fine).reshape(256, half).astype(BF)
        rel = dot(sines, weight_ref[:half]) + dot(cosines, weight_ref[half:])
        out_ref[block * 256 : (block + 1) * 256] = rel.astype(BF)


def reversed_position_keys(length, features, w_rel):
    frequency = 10000.0 ** (-jnp.arange(0, features, 2).astype(F32) / features)
    coarse = (jnp.arange(length // STEP)[::-1] * STEP).astype(F32)[:, None] * frequency[None]
    fine = jnp.arange(STEP)[::-1].astype(F32)[:, None] * frequency[None]
    return pl.pallas_call(
        rel_kernel,
        out_shape=jax.ShapeDtypeStruct((length, w_rel.shape[1]), BF),
        name="rel_keys",
    )(
        jnp.stack([jnp.sin(coarse), jnp.cos(coarse)]),
        jnp.stack([jnp.sin(fine), jnp.cos(fine)]),
        w_rel,
    )


def head_mask(width, head_dim, head):
    lanes = lax.broadcasted_iota(jnp.int32, (1, width), 1)
    return (lanes >= head * head_dim) & (lanes < (head + 1) * head_dim)


def now_kernel(head_dim, qc_ref, qp_ref, key_ref, value_ref, rel_ref, pos_ref, top_ref, total_ref, acc_ref):
    seg_rows, width = qc_ref.shape
    span = rel_ref.shape[0]
    for block in range(seg_rows // ROWS):
        first = block * ROWS
        rows = slice(first, first + ROWS)
        keys = first + ROWS
        columns = lax.broadcasted_iota(jnp.int32, (ROWS, keys), 1)
        causal = columns <= lax.broadcasted_iota(jnp.int32, (ROWS, keys), 0) + first
        acc = jnp.zeros((ROWS, width), F32)
        for head in range(width // head_dim):
            mask = head_mask(width, head_dim, head)
            with_content = jnp.where(mask, qc_ref[rows], 0)
            with_position = jnp.where(mask, qp_ref[rows], 0)
            skewed = dot_nt(with_position, rel_ref[...])
            position = pltpu.roll(skewed, (seg_rows + 1 + first) % span, 1, stride=1, stride_axis=0)
            pos_ref[head, rows] = position[:, :seg_rows]
            score = dot_nt(with_content, key_ref[:keys]) + position[:, seg_rows : seg_rows + keys]
            score = jnp.where(causal, score, MASKED)
            top = jnp.max(score, axis=1, keepdims=True)
            weight = jnp.exp(score - top)
            top_ref[rows, head : head + 1] = top
            total_ref[rows, head : head + 1] = jnp.sum(weight, axis=1, keepdims=True)
            acc = jnp.where(mask, dot(weight.astype(BF), value_ref[:keys]), acc)
        acc_ref[rows] = acc


def past_kernel(head_dim, flag_ref, qc_ref, key_ref, value_ref, pos_ref, top_ref, total_ref, acc_ref, out_ref):
    seg_rows, width = qc_ref.shape
    present = flag_ref[0] >= 0
    for block in range(seg_rows // ROWS):
        rows = slice(block * ROWS, (block + 1) * ROWS)
        out = jnp.zeros((ROWS, width), F32)
        for head in range(width // head_dim):
            mask = head_mask(width, head_dim, head)
            with_content = jnp.where(mask, qc_ref[rows], 0)
            score = dot_nt(with_content, key_ref[...]) + pos_ref[head, rows]
            score = jnp.where(present, score, MASKED)
            now_top = top_ref[rows, head : head + 1]
            top = jnp.maximum(now_top, jnp.max(score, axis=1, keepdims=True))
            weight = jnp.exp(score - top)
            decay = jnp.exp(now_top - top)
            total = total_ref[rows, head : head + 1] * decay + jnp.sum(weight, axis=1, keepdims=True)
            mixed = acc_ref[rows] * decay + dot(weight.astype(BF), value_ref[...])
            out = jnp.where(mask, mixed / total, out)
        out_ref[rows] = out.astype(BF)


def attend(with_content, with_position, key_now, value_now, rel_keys, fetch, pred, head_dim):
    seg_rows, width = with_content.shape
    heads = width // head_dim
    stats = jax.ShapeDtypeStruct((seg_rows, 128), F32)
    local = pl.pallas_call(
        lambda *refs: now_kernel(head_dim, *refs),
        out_shape=(
            jax.ShapeDtypeStruct((heads, seg_rows, seg_rows), F32),
            stats,
            stats,
            jax.ShapeDtypeStruct((seg_rows, width), F32),
        ),
        name="attend_now",
    )(with_content, with_position, key_now, value_now, rel_keys)
    key_past, value_past = fetch
    vmem = pl.BlockSpec(memory_space=pltpu.VMEM)
    return pl.pallas_call(
        lambda *refs: past_kernel(head_dim, *refs),
        out_shape=jax.ShapeDtypeStruct((seg_rows, width), BF),
        in_specs=[pl.BlockSpec(memory_space=pltpu.SMEM)] + [vmem] * 7,
        name="attend_past",
    )(pred, with_content, key_past, value_past, *local)


def fetch_past(payloads, pred):
    count = lax.axis_size("seg")
    index = lax.axis_index("seg")
    odd = index % 2 == 1
    behind = index - pred[0]
    onward = [(k, k + (1 if k % 2 else 3)) for k in range(count)]
    onward = [(k, j) for k, j in onward if j < count]
    wanted = lax.ppermute(behind, "seg", [(j, k) for k, j in onward])
    pair = [swapped(p, "seg", 1) for p in payloads]
    older = [lax.ppermute(p, "seg", [(k, k + 2) for k in range(1, count - 2, 2)]) for p in payloads]
    fetched = []
    for own, other, old in zip(payloads, pair, older):
        passed = jnp.where(
            odd,
            jnp.where(wanted == 1, own, jnp.where(wanted == 2, other, old)),
            jnp.where(wanted == 3, own, other),
        )
        ahead = lax.ppermute(passed, "seg", onward)
        back = lax.ppermute(other, "seg", [(k, k - 2) for k in range(3, count, 2)])
        fetched.append(
            jnp.where(
                odd,
                jnp.where(behind == -1, back, jnp.where(behind == 1, other, ahead)),
                jnp.where(behind == -1, other, ahead),
            )
        )
    return fetched


def gathered(block, axis):
    blocks = [block]
    distance = lax.axis_size(axis) // 2
    far = {0: block}
    while distance >= 1:
        far = {**far, **{d | distance: swapped(b, axis, distance) for d, b in far.items()}}
        distance //= 2
    return [far[d] for d in range(lax.axis_size(axis))]


def mid_kernel(parts, half_ref, *refs):
    heads = refs[:parts]
    outs = refs[parts : 2 * parts]
    (embedded, gain, shift, w_up, up_bias, w_down, partial_ref, first_ref) = refs[2 * parts :]
    total = embedded[...].astype(F32)
    for head, out in zip(heads, outs):
        total = total + dot(head[...], out[...]).astype(BF).astype(F32)
    first = normalize(total, gain[...], shift[...]).astype(BF)
    first_ref[...] = first
    units = jnp.maximum(dot(first, w_up[...]) + up_bias[...], 0.0).astype(BF)
    partial_ref[...] = dot(units, w_down[...]).astype(BF)


def feed_forward(half, attended, outs, embedded, gain, shift, w_up, up_bias, w_down):
    seg_rows, features = embedded.shape
    blocks = seg_rows // 2 // ROWS
    parts = len(attended)
    piece = lambda a: pl.BlockSpec((ROWS, a.shape[1]), lambda i, h: (h[0] * blocks + i, 0))
    whole = lambda a: full(a.shape)
    result = pl.BlockSpec((ROWS, features), lambda i, h: (i, 0))
    return pl.pallas_call(
        lambda *refs: mid_kernel(parts, *refs),
        grid_spec=pltpu.PrefetchScalarGridSpec(
            num_scalar_prefetch=1,
            grid=(blocks,),
            in_specs=[piece(a) for a in attended]
            + [whole(o) for o in outs]
            + [piece(embedded)]
            + [whole(a) for a in (gain, shift, w_up, up_bias, w_down)],
            out_specs=[result, result],
        ),
        out_shape=(jax.ShapeDtypeStruct((seg_rows // 2, features), BF),) * 2,
        name="feed_forward",
    )(half, *attended, *outs, embedded, gain, shift, w_up, up_bias, w_down)


def second_kernel(count, *refs):
    terms = refs[:count]
    first, bias, gain, shift, out_ref = refs[count:]
    total = first[...].astype(F32) + bias[...]
    for term in terms:
        total = total + term[...].astype(F32)
    out_ref[...] = normalize(total, gain[...], shift[...]).astype(BF)


def vocab_kernel(rows_ref, w_ref, ids_ref, out_ref, logits_ref):
    count = rows_ref.shape[0]
    words = w_ref.shape[1]
    rows = rows_ref[...]
    ids = ids_ref[...]
    lanes = lax.broadcasted_iota(jnp.int32, (count, 128), 1)
    chunk = 512
    tops = None
    for start in range(0, words, chunk):
        logits = dot(rows, w_ref[:, start : start + chunk])
        logits_ref[:, start : start + chunk] = logits
        for at in range(0, chunk, 128):
            piece = logits[:, at : at + 128]
            tops = piece if tops is None else jnp.maximum(tops, piece)
    top = jnp.max(tops, axis=1, keepdims=True)
    total = jnp.zeros((count, 128), F32)
    picked = jnp.zeros((count, 128), F32)
    for start in range(0, words, 128):
        piece = logits_ref[:, start : start + 128]
        total = total + jnp.exp(piece - top)
        picked = picked + jnp.where(lanes == ids - start, piece, 0.0)
    total = jnp.sum(total, axis=1, keepdims=True)
    picked = jnp.sum(picked, axis=1, keepdims=True)
    packed = jnp.where(lanes == 0, top, jnp.where(lanes == 1, total, picked))
    out_ref[...] = packed.T[:8]


def vocab_stats(rows, w_vocab, ids):
    count = rows.shape[0]
    return pl.pallas_call(
        vocab_kernel,
        out_shape=jax.ShapeDtypeStruct((8, count), F32),
        scratch_shapes=[pltpu.VMEM((count, w_vocab.shape[1]), F32)],
        name="vocab_stats",
    )(rows, w_vocab, ids)


def on_device(
    embedded,
    targets,
    pred_device,
    doc_ids,
    valid_rows,
    w_query,
    w_key,
    w_value,
    w_rel,
    content_bias,
    position_bias,
    attn_out,
    attn_gain,
    attn_shift,
    w_up,
    up_bias,
    w_down,
    down_bias,
    ffn_gain,
    ffn_shift,
    w_vocab,
):
    seg_rows, features = embedded.shape
    head_dim = content_bias.shape[1]
    score_scale = head_dim ** (-0.5)
    row = lambda a: a.reshape(1, -1)
    key_now = dot(embedded, w_key).astype(BF)
    value_now = dot(embedded, w_value).astype(BF)
    fetch = fetch_past([key_now, value_now], pred_device)
    outs = gathered(attn_out, "mp")
    queries = dot(embedded, w_query)
    with_content = (queries + row(content_bias)).astype(BF) * BF(score_scale)
    with_position = (queries + row(position_bias)).astype(BF) * BF(score_scale)
    rel_keys = reversed_position_keys(2 * seg_rows, features, w_rel)
    attended = attend(
        with_content, with_position, key_now, value_now, rel_keys, fetch, pred_device, head_dim
    )
    attended = gathered(attended, "mp")
    mp_count = lax.axis_size("mp")
    mp_index = lax.axis_index("mp")
    mine = (mp_index % 2).astype(jnp.int32)
    forward = lambda half: feed_forward(
        half.reshape(1),
        attended,
        outs,
        embedded,
        row(attn_gain),
        row(attn_shift),
        w_up,
        row(up_bias),
        w_down,
    )
    given, _ = forward(1 - mine)
    kept, first_out = forward(mine)
    terms = [kept, swapped(given, "mp", 1)]
    distance = 2
    while distance < mp_count:
        terms = [(terms[0].astype(F32) + terms[1].astype(F32)).astype(BF)]
        terms.append(swapped(terms[0], "mp", distance))
        distance *= 2
    second = pl.pallas_call(
        lambda *refs: second_kernel(len(terms), *refs),
        out_shape=jax.ShapeDtypeStruct(first_out.shape, BF),
        name="second",
    )(*terms, first_out, row(down_bias), row(ffn_gain), row(ffn_shift))
    other = swapped(second, "mp", 1)
    ids = (targets - mp_index * w_vocab.shape[1]).reshape(2, seg_rows // 2, 1)
    ids_of = lambda half: lax.dynamic_index_in_dim(ids, half, 0, False)
    stats_mine = vocab_stats(second, w_vocab, ids_of(mine))
    stats_other = vocab_stats(other, w_vocab, ids_of(1 - mine))
    low = jnp.where(mine == 0, stats_mine, stats_other)
    high = jnp.where(mine == 0, stats_other, stats_mine)
    stats = lax.all_gather(jnp.concatenate([low[:3], high[:3]], axis=0), "mp")
    stats = stats.reshape(mp_count, 2, 3, seg_rows // 2)
    top = jnp.max(stats[:, :, 0], axis=0)
    total = jnp.sum(stats[:, :, 1] * jnp.exp(stats[:, :, 0] - top[None]), axis=0)
    token_terms = jnp.sum(stats[:, :, 2], axis=0) - (top + jnp.log(total))
    token_terms = token_terms.reshape(seg_rows)
    token_terms = jnp.where(jnp.arange(seg_rows) < valid_rows[0], token_terms, 0.0)
    doc_slots = lax.axis_size("seg") // DOC_SPAN
    marker = jnp.arange(doc_slots) == doc_ids[0]
    pair = jnp.stack([jnp.sum(token_terms), valid_rows[0].astype(F32)])
    sums = jnp.where(marker[None], pair[:, None], 0.0)
    distance = 1
    while distance < lax.axis_size("seg"):
        sums = sums + swapped(sums, "seg", distance)
        distance *= 2
    return (token_terms, sums[0] / sums[1])


def solution(mesh):
    return jax.shard_map(
        on_device,
        mesh=mesh,
        in_specs=(
            P("seg", None),
            P("seg"),
            P("seg"),
            P("seg"),
            P("seg"),
            P(None, "mp"),
            P(None, "mp"),
            P(None, "mp"),
            P(None, "mp"),
            P("mp", None),
            P("mp", None),
            P("mp", None),
            P(),
            P(),
            P(None, "mp"),
            P("mp"),
            P("mp", None),
            P(),
            P(),
            P(),
            P(None, "mp"),
        ),
        out_specs=(P("seg"), P()),
        check_vma=False,
    )
```

```python
import jax
import jax.numpy as jnp
from jax import lax
from jax.experimental import pallas as pl
from jax.experimental.pallas import tpu as pltpu
from jax.sharding import PartitionSpec as P

DOC_SPAN = 4
EPSILON = 1e-05
STEP = 32
ROWS = 256
PARTS = 4
MASKED = -1e30
BF = jnp.bfloat16
F32 = jnp.float32


def swapped(block, axis, distance):
    return lax.ppermute(block, axis, [(i, i ^ distance) for i in range(lax.axis_size(axis))])


def dot(a, b):
    return jnp.dot(a, b, preferred_element_type=F32)


def near(a):
    return pltpu.with_memory_space_constraint(a, pltpu.MemorySpace.VMEM)


def afar(a):
    return pltpu.with_memory_space_constraint(a, pltpu.MemorySpace.HBM)


def room(mebibytes):
    return pltpu.CompilerParams(vmem_limit_bytes=mebibytes << 20)


IN_VMEM = pl.BlockSpec(memory_space=pltpu.VMEM)
IN_SMEM = pl.BlockSpec(memory_space=pltpu.SMEM)
IN_PLACE = pl.BlockSpec(memory_space=pltpu.MemorySpace.HBM)


def chunk_copies(source, target, sems, parts):
    rows = source.shape[0] // parts
    return [
        pltpu.make_async_copy(
            source.at[pl.ds(k * rows, rows)], target.at[pl.ds(k * rows, rows)], sems.at[k]
        )
        for k in range(parts)
    ]


def kv_kernel(embedded_ref, key_ref, value_ref, out_ref, rows_ref, key_near, value_near, sems):
    seg_rows = embedded_ref.shape[0]
    loads = [
        chunk_copies(source, target, sems.at[k], PARTS)
        for k, (source, target) in enumerate(
            [(key_ref, key_near), (embedded_ref, rows_ref), (value_ref, value_near)]
        )
    ]
    for copies in loads:
        for copy in copies:
            copy.start()
    for copy in loads[0] + loads[1]:
        copy.wait()
    out_ref[:seg_rows] = dot(rows_ref[...], key_near[...]).astype(BF)
    for copy in loads[2]:
        copy.wait()
    out_ref[seg_rows:] = dot(rows_ref[...], value_near[...]).astype(BF)


def keys_and_values(embedded, w_key, w_value):
    return pl.pallas_call(
        kv_kernel,
        out_shape=jax.ShapeDtypeStruct((2 * embedded.shape[0], w_key.shape[1]), BF),
        in_specs=[IN_PLACE] * 3,
        out_specs=IN_VMEM,
        scratch_shapes=[
            pltpu.VMEM(embedded.shape, BF),
            pltpu.VMEM(w_key.shape, BF),
            pltpu.VMEM(w_value.shape, BF),
            pltpu.SemaphoreType.DMA((3, PARTS)),
        ],
        compiler_params=room(12),
        name="keys_and_values",
    )(afar(embedded), afar(w_key), afar(w_value))


def load_kernel(count, *refs):
    sources, targets, sems = refs[:count], refs[count + 1 : 2 * count + 1], refs[2 * count + 1]
    copies = []
    for k, (source, target) in enumerate(zip(sources, targets)):
        copies += chunk_copies(source, target, sems.at[k], PARTS)
    for copy in copies:
        copy.start()
    for copy in copies:
        copy.wait()


def load(weights, after):
    count = len(weights)
    return pl.pallas_call(
        lambda *refs: load_kernel(count, *refs),
        out_shape=[jax.ShapeDtypeStruct(w.shape, w.dtype) for w in weights],
        in_specs=[IN_PLACE] * count + [pl.BlockSpec(memory_space=pl.ANY)],
        out_specs=[IN_VMEM] * count,
        scratch_shapes=[pltpu.SemaphoreType.DMA((count, PARTS))],
        compiler_params=room(4),
        name="load",
    )(*[afar(w) for w in weights], after)


def turned(a):
    return a.astype(F32).T.astype(BF)


def normalize(values, norm_gain, norm_shift):
    centre = values - jnp.mean(values, axis=-1, keepdims=True)
    spread = jnp.mean(centre * centre, axis=-1, keepdims=True)
    return centre * lax.rsqrt(spread + EPSILON) * norm_gain + norm_shift


def prepare_kernel(scale, *refs):
    rows_ref, query_ref, content_ref, position_ref, coarse_ref, fine_ref, weight_ref, targets_ref = refs[:8]
    qc_ref, qp_ref, out_ref, halves_ref, done_ref = refs[8:]
    halves_ref[...] = targets_ref[...]
    done_ref[0] = 0
    queries = dot(rows_ref[...], query_ref[...])
    qc_ref[...] = (queries + content_ref[...]).astype(BF) * BF(scale)
    qp_ref[...] = (queries + position_ref[...]).astype(BF) * BF(scale)
    half = coarse_ref.shape[2]
    group = 256 // STEP
    sin_fine = fine_ref[0][None]
    cos_fine = fine_ref[1][None]
    for block in range(coarse_ref.shape[1] // group):
        sin_coarse = coarse_ref[0, block * group : (block + 1) * group][:, None]
        cos_coarse = coarse_ref[1, block * group : (block + 1) * group][:, None]
        sines = (sin_coarse * cos_fine + cos_coarse * sin_fine).reshape(256, half).astype(BF)
        cosines = (cos_coarse * cos_fine - sin_coarse * sin_fine).reshape(256, half).astype(BF)
        rel = dot(sines, weight_ref[:half]) + dot(cosines, weight_ref[half:])
        out_ref[:, block * 256 : (block + 1) * 256] = rel.T.astype(BF)


def prepare(embedded, w_query, content_bias, position_bias, w_rel, targets, scale):
    seg_rows, features = embedded.shape
    length = 2 * seg_rows
    width = w_query.shape[1]
    frequency = 10000.0 ** (-jnp.arange(0, features, 2).astype(F32) / features)
    coarse = (jnp.arange(length // STEP)[::-1] * STEP).astype(F32)[:, None] * frequency[None]
    fine = jnp.arange(STEP)[::-1].astype(F32)[:, None] * frequency[None]
    queries = jax.ShapeDtypeStruct((seg_rows, width), BF)
    return pl.pallas_call(
        lambda *refs: prepare_kernel(scale, *refs),
        out_shape=(
            queries,
            queries,
            jax.ShapeDtypeStruct((width, length), BF),
            jax.ShapeDtypeStruct((2, seg_rows // 2), jnp.int32),
            jax.ShapeDtypeStruct((1,), jnp.int32),
        ),
        in_specs=[IN_VMEM] * 8,
        out_specs=[IN_VMEM] * 4 + [IN_SMEM],
        compiler_params=room(12),
        name="prepare",
    )(
        near(embedded),
        near(w_query),
        content_bias,
        position_bias,
        near(jnp.stack([jnp.sin(coarse), jnp.cos(coarse)])),
        near(jnp.stack([jnp.sin(fine), jnp.cos(fine)])),
        near(w_rel),
        targets.reshape(2, seg_rows // 2),
    )


def head_lanes(width, head_dim):
    lanes = min(width, max(128, head_dim))
    at = lax.broadcasted_iota(jnp.int32, (1, lanes), 1)
    for head in range(width // head_dim):
        start = head * head_dim // lanes * lanes
        first = head * head_dim - start
        yield head, slice(start, start + lanes), (at >= first) & (at < first + head_dim)


def now_kernel(head_dim, *refs):
    qc_ref, qp_ref, own_ref, rel_ref, pos_ref, top_ref, total_ref, acc_ref, key_ref = refs
    seg_rows, width = qc_ref.shape
    span = rel_ref.shape[1]
    key_ref[...] = turned(own_ref[:seg_rows])
    for block in range(seg_rows // ROWS):
        first = block * ROWS
        rows = slice(first, first + ROWS)
        keys = first + ROWS
        columns = lax.broadcasted_iota(jnp.int32, (ROWS, keys), 1)
        causal = columns <= lax.broadcasted_iota(jnp.int32, (ROWS, keys), 0) + first
        for head, lanes, mask in head_lanes(width, head_dim):
            with_content = jnp.where(mask, qc_ref[rows, lanes], 0)
            with_position = jnp.where(mask, qp_ref[rows, lanes], 0)
            skewed = dot(with_position, rel_ref[lanes])
            position = pltpu.roll(skewed, (seg_rows + 1 + first) % span, 1, stride=1, stride_axis=0)
            pos_ref[head, rows] = position[:, :seg_rows]
            score = dot(with_content, key_ref[lanes, :keys]) + position[:, seg_rows : seg_rows + keys]
            score = jnp.where(causal, score, MASKED)
            top = jnp.max(score, axis=1, keepdims=True)
            weight = jnp.exp(score - top)
            top_ref[rows, head : head + 1] = top
            total_ref[rows, head : head + 1] = jnp.sum(weight, axis=1, keepdims=True)
            mixed = dot(weight.astype(BF), own_ref[seg_rows : seg_rows + keys, lanes])
            old = acc_ref[rows, lanes] if head * head_dim > lanes.start else 0.0
            acc_ref[rows, lanes] = jnp.where(mask, mixed, old)


def past_kernel(head_dim, pred_ref, *refs):
    qc_ref, pair_ref, ahead_ref, back_ref, pos_ref, top_ref, total_ref, acc_ref = refs[:8]
    out_ref, key_ref, value_ref = refs[8:]
    seg_rows, width = qc_ref.shape
    index = lax.axis_index("seg")
    present = pred_ref[0] >= 0
    behind = index - pred_ref[0]
    in_pair = behind == 2 * (index % 2) - 1
    for start in (0, seg_rows):
        part = slice(start, start + seg_rows)
        chosen = jnp.where(behind == -1, back_ref[part], ahead_ref[part])
        chosen = jnp.where(in_pair, pair_ref[part], chosen)
        if start:
            value_ref[...] = chosen
        else:
            key_ref[...] = turned(chosen)
    for block in range(seg_rows // ROWS):
        rows = slice(block * ROWS, (block + 1) * ROWS)
        out = {}
        for head, lanes, mask in head_lanes(width, head_dim):
            with_content = jnp.where(mask, qc_ref[rows, lanes], 0)
            score = dot(with_content, key_ref[lanes]) + pos_ref[head, rows]
            score = jnp.where(present, score, MASKED)
            now_top = top_ref[rows, head : head + 1]
            top = jnp.maximum(now_top, jnp.max(score, axis=1, keepdims=True))
            weight = jnp.exp(score - top)
            decay = jnp.exp(now_top - top)
            total = total_ref[rows, head : head + 1] * decay + jnp.sum(weight, axis=1, keepdims=True)
            mixed = acc_ref[rows, lanes] * decay + dot(weight.astype(BF), value_ref[:, lanes])
            mixed = mixed * (1.0 / total)
            old = out.get(lanes.start, 0.0)
            out[lanes.start] = jnp.where(mask, mixed, old)
        for start, value in out.items():
            out_ref[rows, start : start + value.shape[1]] = value.astype(BF)


def attend_now(with_content, with_position, own, rel_keys, head_dim):
    seg_rows, width = with_content.shape
    heads = width // head_dim
    stats = jax.ShapeDtypeStruct((seg_rows, 128), F32)
    return pl.pallas_call(
        lambda *refs: now_kernel(head_dim, *refs),
        out_shape=(
            jax.ShapeDtypeStruct((heads, seg_rows, seg_rows), F32),
            stats,
            stats,
            jax.ShapeDtypeStruct((seg_rows, width), F32),
        ),
        in_specs=[IN_VMEM] * 4,
        out_specs=[IN_VMEM] * 4,
        scratch_shapes=[pltpu.VMEM((width, seg_rows), BF)],
        compiler_params=room(12),
        name="attend_now",
    )(*[near(a) for a in (with_content, with_position, own, rel_keys)])


def attend_past(pred, with_content, sources, local, head_dim):
    seg_rows, width = with_content.shape
    return pl.pallas_call(
        lambda *refs: past_kernel(head_dim, *refs),
        out_shape=jax.ShapeDtypeStruct((seg_rows, width), BF),
        in_specs=[IN_SMEM] + [IN_VMEM] * 8,
        out_specs=IN_VMEM,
        scratch_shapes=[pltpu.VMEM((width, seg_rows), BF), pltpu.VMEM((seg_rows, width), BF)],
        compiler_params=room(12),
        name="attend_past",
    )(pred, *[near(a) for a in (with_content, *sources, *local)])


def fetch_first(own, behind):
    count = lax.axis_size("seg")
    onward = [(k, k + (1 if k % 2 else 3)) for k in range(count)]
    onward = [(k, j) for k, j in onward if j < count]
    pair = swapped(own, "seg", 1)
    older = lax.ppermute(own, "seg", [(k, k + 2) for k in range(1, count - 2, 2)])
    wanted = lax.ppermute(behind, "seg", [(j, k) for k, j in onward])
    return pair, older, wanted, onward


def choose_kernel(wanted_ref, done_ref, own_ref, pair_ref, older_ref, out_ref):
    odd = lax.axis_index("seg") % 2
    wanted = wanted_ref[0] + done_ref[0]
    use_own = wanted == 3 - 2 * odd
    use_older = (odd == 1) & (wanted == 3)
    out_ref[...] = jnp.where(use_own, own_ref[...], jnp.where(use_older, older_ref[...], pair_ref[...]))


def fetch_second(own, pair, older, wanted, done, onward):
    count = lax.axis_size("seg")
    passed = pl.pallas_call(
        choose_kernel,
        out_shape=jax.ShapeDtypeStruct(own.shape, BF),
        in_specs=[IN_SMEM] * 2 + [IN_VMEM] * 3,
        out_specs=IN_VMEM,
        compiler_params=room(8),
        name="choose",
    )(wanted, done, near(own), near(pair), near(older))
    ahead = lax.ppermute(passed, "seg", onward)
    back = lax.ppermute(pair, "seg", [(k, k - 2) for k in range(3, count, 2)])
    return ahead, back


def gathered(block, axis):
    distance = lax.axis_size(axis) // 2
    far = {0: block}
    while distance >= 1:
        far = {**far, **{d | distance: swapped(b, axis, distance) for d, b in far.items()}}
        distance //= 2
    return [far[d] for d in range(lax.axis_size(axis))]


def mid_kernel(parts, role, *refs):
    heads = refs[:parts]
    outs = refs[parts : 2 * parts]
    (embedded, gain, shift, w_up, up_bias, w_down, partial_ref, first_ref) = refs[2 * parts :]
    count = partial_ref.shape[0]
    half = (lax.axis_index("mp") + role) % 2
    for block in range(count // ROWS):
        rows = pl.ds(pl.multiple_of(half * count + block * ROWS, ROWS), ROWS)
        put = slice(block * ROWS, (block + 1) * ROWS)
        total = embedded[rows].astype(F32)
        for head, out in zip(heads, outs):
            total = total + dot(head[rows], out[...]).astype(BF).astype(F32)
        first = normalize(total, gain[...], shift[...]).astype(BF)
        first_ref[put] = first
        units = jnp.maximum(dot(first, w_up[...]) + up_bias[...], 0.0).astype(BF)
        partial_ref[put] = dot(units, w_down[...]).astype(BF)


def feed_forward(role, attended, outs, embedded, gain, shift, w_up, up_bias, w_down):
    seg_rows, features = embedded.shape
    parts = len(attended)
    return pl.pallas_call(
        lambda *refs: mid_kernel(parts, role, *refs),
        in_specs=[IN_VMEM] * (2 * parts + 6),
        out_specs=[IN_VMEM, IN_VMEM],
        out_shape=(jax.ShapeDtypeStruct((seg_rows // 2, features), BF),) * 2,
        compiler_params=room(16),
        name="feed_forward",
    )(*[near(a) for a in (*attended, *outs, embedded)], gain, shift, near(w_up), up_bias, near(w_down))


def second_kernel(count, *refs):
    terms = refs[:count]
    first, bias, gain, shift, out_ref = refs[count:]
    total = first[...].astype(F32) + bias[...]
    for term in terms:
        total = total + term[...].astype(F32)
    out_ref[...] = normalize(total, gain[...], shift[...]).astype(BF)


def vocab_kernel(role, rows_ref, w_ref, targets_ref, out_ref, logits_ref):
    count = rows_ref.shape[0]
    words = w_ref.shape[1]
    rows = rows_ref[...]
    index = lax.axis_index("mp")
    ids = jnp.where((index + role) % 2 == 0, targets_ref[0:1], targets_ref[1:2])
    ids = (ids - index * words).astype(F32)
    ids = jnp.broadcast_to(ids, (8, count)).T[:, :1].astype(jnp.int32)
    lanes = lax.broadcasted_iota(jnp.int32, (count, 128), 1)
    chunk = 512
    tops = None
    for start in range(0, words, chunk):
        logits = dot(rows, w_ref[:, start : start + chunk])
        logits_ref[:, start : start + chunk] = logits
        for at in range(0, chunk, 128):
            piece = logits[:, at : at + 128]
            tops = piece if tops is None else jnp.maximum(tops, piece)
    top = jnp.max(tops, axis=1, keepdims=True)
    total = jnp.zeros((count, 128), F32)
    picked = jnp.zeros((count, 128), F32)
    for start in range(0, words, 128):
        piece = logits_ref[:, start : start + 128]
        total = total + jnp.exp(piece - top)
        picked = picked + jnp.where(lanes == ids - start, piece, 0.0)
    total = jnp.sum(total, axis=1, keepdims=True)
    picked = jnp.sum(picked, axis=1, keepdims=True)
    packed = jnp.where(lanes == 0, top, jnp.where(lanes == 1, total, picked))
    out_ref[...] = packed.T[:8]


def vocab_stats(role, rows, w_vocab, targets):
    count = rows.shape[0]
    return pl.pallas_call(
        lambda *refs: vocab_kernel(role, *refs),
        in_specs=[IN_VMEM] * 3,
        out_specs=IN_VMEM,
        out_shape=jax.ShapeDtypeStruct((8, count), F32),
        scratch_shapes=[pltpu.VMEM((count, w_vocab.shape[1]), F32)],
        compiler_params=room(16),
        name="vocab_stats",
    )(near(rows), near(w_vocab), targets)


def on_device(
    embedded,
    targets,
    pred_device,
    doc_ids,
    valid_rows,
    w_query,
    w_key,
    w_value,
    w_rel,
    content_bias,
    position_bias,
    attn_out,
    attn_gain,
    attn_shift,
    w_up,
    up_bias,
    w_down,
    down_bias,
    ffn_gain,
    ffn_shift,
    w_vocab,
):
    seg_rows, _ = embedded.shape
    head_dim = content_bias.shape[1]
    score_scale = head_dim ** (-0.5)
    row = lambda a: a.reshape(1, -1)
    behind = lax.axis_index("seg") - pred_device
    own = keys_and_values(embedded, w_key, w_value)
    pair, older, wanted, onward = fetch_first(own, behind)
    with_content, with_position, rel_keys, halves, done = prepare(
        embedded, w_query, row(content_bias), row(position_bias), w_rel, targets, score_scale
    )
    local = attend_now(with_content, with_position, own, rel_keys, head_dim)
    ahead, back = fetch_second(own, pair, older, wanted, done, onward)
    outs = gathered(attn_out, "mp")
    attended = attend_past(pred_device, with_content, (pair, ahead, back), local, head_dim)
    w_up, w_down = load([w_up, w_down], attended)
    attended = gathered(attended, "mp")
    mp_count = lax.axis_size("mp")
    forward = lambda role: feed_forward(
        role,
        attended,
        outs,
        embedded,
        row(attn_gain),
        row(attn_shift),
        w_up,
        row(up_bias),
        w_down,
    )
    given, _ = forward(1)
    kept, first_out = forward(0)
    (w_vocab,) = load([w_vocab], kept)
    terms = [kept, swapped(given, "mp", 1)]
    distance = 2
    while distance < mp_count:
        terms = [(terms[0].astype(F32) + terms[1].astype(F32)).astype(BF)]
        terms.append(swapped(terms[0], "mp", distance))
        distance *= 2
    second = pl.pallas_call(
        lambda *refs: second_kernel(len(terms), *refs),
        out_shape=jax.ShapeDtypeStruct(first_out.shape, BF),
        compiler_params=room(8),
        name="second",
    )(*[near(t) for t in terms], near(first_out), row(down_bias), row(ffn_gain), row(ffn_shift))
    other = swapped(second, "mp", 1)
    stats_mine = vocab_stats(0, second, w_vocab, halves)
    stats_other = vocab_stats(1, other, w_vocab, halves)
    stats = lax.all_gather(jnp.concatenate([stats_mine[:3], stats_other[:3]], axis=0), "mp")
    stats = stats.reshape(mp_count, 2, 3, seg_rows // 2)
    stats = jnp.stack([stats[k, :: 1 - 2 * (k % 2)] for k in range(mp_count)])
    top = jnp.max(stats[:, :, 0], axis=0)
    total = jnp.sum(stats[:, :, 1] * jnp.exp(stats[:, :, 0] - top[None]), axis=0)
    token_terms = jnp.sum(stats[:, :, 2], axis=0) - (top + jnp.log(total))
    token_terms = token_terms.reshape(seg_rows)
    token_terms = jnp.where(jnp.arange(seg_rows) < valid_rows[0], token_terms, 0.0)
    doc_slots = lax.axis_size("seg") // DOC_SPAN
    marker = jnp.arange(doc_slots) == doc_ids[0]
    pair = jnp.stack([jnp.sum(token_terms), valid_rows[0].astype(F32)])
    sums = jnp.where(marker[None], pair[:, None], 0.0)
    distance = 1
    while distance < lax.axis_size("seg"):
        wide = distance > 1 and 4 * distance <= lax.axis_size("seg")
        steps = (1, 2, 3) if wide else (1,)
        sums = sum([swapped(sums, "seg", distance * step) for step in steps], sums)
        distance *= 1 + len(steps)
    return (token_terms, sums[0] / sums[1])


def solution(mesh):
    return jax.shard_map(
        on_device,
        mesh=mesh,
        in_specs=(
            P("seg", None),
            P("seg"),
            P("seg"),
            P("seg"),
            P("seg"),
            P(None, "mp"),
            P(None, "mp"),
            P(None, "mp"),
            P(None, "mp"),
            P("mp", None),
            P("mp", None),
            P("mp", None),
            P(),
            P(),
            P(None, "mp"),
            P("mp"),
            P("mp", None),
            P(),
            P(),
            P(),
            P(None, "mp"),
        ),
        out_specs=(P("seg"), P()),
        check_vma=False,
    )
```

```python
import jax
import jax.numpy as jnp
from jax import lax
from jax.experimental import pallas as pl
from jax.experimental.pallas import tpu as pltpu
from jax.sharding import PartitionSpec as P

DOC_SPAN = 4
EPSILON = 1e-05
STEP = 32
ROWS = 256
PARTS = 4
MASKED = -1e30
BF = jnp.bfloat16
F32 = jnp.float32


def swapped(block, axis, distance):
    return lax.ppermute(block, axis, [(i, i ^ distance) for i in range(lax.axis_size(axis))])


def dot(a, b):
    return jnp.dot(a, b, preferred_element_type=F32)


def near(a):
    return pltpu.with_memory_space_constraint(a, pltpu.MemorySpace.VMEM)


def afar(a):
    return pltpu.with_memory_space_constraint(a, pltpu.MemorySpace.HBM)


def room(mebibytes):
    return pltpu.CompilerParams(vmem_limit_bytes=mebibytes << 20)


IN_VMEM = pl.BlockSpec(memory_space=pltpu.VMEM)
IN_SMEM = pl.BlockSpec(memory_space=pltpu.SMEM)
IN_PLACE = pl.BlockSpec(memory_space=pltpu.MemorySpace.HBM)


def chunk_copies(source, target, sems, parts):
    rows = source.shape[0] // parts
    return [
        pltpu.make_async_copy(
            source.at[pl.ds(k * rows, rows)], target.at[pl.ds(k * rows, rows)], sems.at[k]
        )
        for k in range(parts)
    ]


def kv_kernel(embedded_ref, key_ref, value_ref, out_ref, rows_ref, key_near, value_near, sems):
    seg_rows = embedded_ref.shape[0]
    loads = [
        chunk_copies(source, target, sems.at[k], PARTS)
        for k, (source, target) in enumerate(
            [(key_ref, key_near), (embedded_ref, rows_ref), (value_ref, value_near)]
        )
    ]
    for copies in loads:
        for copy in copies:
            copy.start()
    for copy in loads[0]:
        copy.wait()
    half = seg_rows // 2
    for k in range(2):
        for copy in loads[1][k * PARTS // 2 : (k + 1) * PARTS // 2]:
            copy.wait()
        part = slice(k * half, (k + 1) * half)
        out_ref[part] = dot(rows_ref[part], key_near[...]).astype(BF)
    for copy in loads[2]:
        copy.wait()
    out_ref[seg_rows:] = dot(rows_ref[...], value_near[...]).astype(BF)


def keys_and_values(embedded, w_key, w_value):
    return pl.pallas_call(
        kv_kernel,
        out_shape=jax.ShapeDtypeStruct((2 * embedded.shape[0], w_key.shape[1]), BF),
        in_specs=[IN_PLACE] * 3,
        out_specs=IN_VMEM,
        scratch_shapes=[
            pltpu.VMEM(embedded.shape, BF),
            pltpu.VMEM(w_key.shape, BF),
            pltpu.VMEM(w_value.shape, BF),
            pltpu.SemaphoreType.DMA((3, PARTS)),
        ],
        compiler_params=room(12),
        name="keys_and_values",
    )(afar(embedded), afar(w_key), afar(w_value))


def load_kernel(count, *refs):
    sources, targets, sems = refs[:count], refs[count + 1 : 2 * count + 1], refs[2 * count + 1]
    copies = []
    for k, (source, target) in enumerate(zip(sources, targets)):
        copies += chunk_copies(source, target, sems.at[k], PARTS)
    for copy in copies:
        copy.start()
    for copy in copies:
        copy.wait()


def load(weights, after):
    count = len(weights)
    return pl.pallas_call(
        lambda *refs: load_kernel(count, *refs),
        out_shape=[jax.ShapeDtypeStruct(w.shape, w.dtype) for w in weights],
        in_specs=[IN_PLACE] * count + [pl.BlockSpec(memory_space=pl.ANY)],
        out_specs=[IN_VMEM] * count,
        scratch_shapes=[pltpu.SemaphoreType.DMA((count, PARTS))],
        compiler_params=room(4),
        name="load",
    )(*[afar(w) for w in weights], after)


def turned(a):
    return a.astype(F32).T.astype(BF)


def normalize(values, norm_gain, norm_shift):
    centre = values - jnp.mean(values, axis=-1, keepdims=True)
    spread = jnp.mean(centre * centre, axis=-1, keepdims=True)
    return centre * lax.rsqrt(spread + EPSILON) * norm_gain + norm_shift


def prepare_kernel(scale, *refs):
    rows_ref, query_ref, content_ref, position_ref, coarse_ref, fine_ref, weight_ref, targets_ref = refs[:8]
    valid_ref, doc_ref, qc_ref, qp_ref, out_ref, halves_ref, facts_ref = refs[8:]
    halves_ref[...] = targets_ref[...]
    facts_ref[0] = 0
    facts_ref[1] = valid_ref[0]
    facts_ref[2] = doc_ref[0]
    queries = dot(rows_ref[...], query_ref[...])
    qc_ref[...] = (queries + content_ref[...]).astype(BF) * BF(scale)
    qp_ref[...] = (queries + position_ref[...]).astype(BF) * BF(scale)
    half = coarse_ref.shape[2]
    group = 256 // STEP
    sin_fine = fine_ref[0][None]
    cos_fine = fine_ref[1][None]
    for block in range(coarse_ref.shape[1] // group):
        sin_coarse = coarse_ref[0, block * group : (block + 1) * group][:, None]
        cos_coarse = coarse_ref[1, block * group : (block + 1) * group][:, None]
        sines = (sin_coarse * cos_fine + cos_coarse * sin_fine).reshape(256, half).astype(BF)
        cosines = (cos_coarse * cos_fine - sin_coarse * sin_fine).reshape(256, half).astype(BF)
        rel = dot(sines, weight_ref[:half]) + dot(cosines, weight_ref[half:])
        out_ref[:, block * 256 : (block + 1) * 256] = rel.T.astype(BF)


def prepare(embedded, w_query, content_bias, position_bias, w_rel, targets, valid_rows, doc_ids, scale):
    seg_rows, features = embedded.shape
    length = 2 * seg_rows
    width = w_query.shape[1]
    frequency = 10000.0 ** (-jnp.arange(0, features, 2).astype(F32) / features)
    coarse = (jnp.arange(length // STEP)[::-1] * STEP).astype(F32)[:, None] * frequency[None]
    fine = jnp.arange(STEP)[::-1].astype(F32)[:, None] * frequency[None]
    queries = jax.ShapeDtypeStruct((seg_rows, width), BF)
    return pl.pallas_call(
        lambda *refs: prepare_kernel(scale, *refs),
        out_shape=(
            queries,
            queries,
            jax.ShapeDtypeStruct((width, length), BF),
            jax.ShapeDtypeStruct((2, seg_rows // 2), jnp.int32),
            jax.ShapeDtypeStruct((3,), jnp.int32),
        ),
        in_specs=[IN_VMEM] * 8 + [IN_SMEM] * 2,
        out_specs=[IN_VMEM] * 4 + [IN_SMEM],
        compiler_params=room(12),
        name="prepare",
    )(
        near(embedded),
        near(w_query),
        content_bias,
        position_bias,
        near(jnp.stack([jnp.sin(coarse), jnp.cos(coarse)])),
        near(jnp.stack([jnp.sin(fine), jnp.cos(fine)])),
        near(w_rel),
        targets.reshape(2, seg_rows // 2),
        valid_rows,
        doc_ids,
    )


def head_lanes(width, head_dim):
    lanes = min(width, max(128, head_dim))
    at = lax.broadcasted_iota(jnp.int32, (1, lanes), 1)
    for head in range(width // head_dim):
        start = head * head_dim // lanes * lanes
        first = head * head_dim - start
        yield head, slice(start, start + lanes), (at >= first) & (at < first + head_dim)


def now_kernel(head_dim, *refs):
    qc_ref, qp_ref, own_ref, rel_ref, pos_ref, top_ref, total_ref, acc_ref, key_ref = refs
    seg_rows, width = qc_ref.shape
    span = rel_ref.shape[1]
    key_ref[...] = turned(own_ref[:seg_rows])
    for block in range(seg_rows // ROWS):
        first = block * ROWS
        rows = slice(first, first + ROWS)
        keys = first + ROWS
        columns = lax.broadcasted_iota(jnp.int32, (ROWS, keys), 1)
        causal = columns <= lax.broadcasted_iota(jnp.int32, (ROWS, keys), 0) + first
        for head, lanes, mask in head_lanes(width, head_dim):
            with_content = jnp.where(mask, qc_ref[rows, lanes], 0)
            with_position = jnp.where(mask, qp_ref[rows, lanes], 0)
            skewed = dot(with_position, rel_ref[lanes])
            position = pltpu.roll(skewed, (seg_rows + 1 + first) % span, 1, stride=1, stride_axis=0)
            pos_ref[head, rows] = position[:, :seg_rows]
            score = dot(with_content, key_ref[lanes, :keys]) + position[:, seg_rows : seg_rows + keys]
            score = jnp.where(causal, score, MASKED)
            top = jnp.max(score, axis=1, keepdims=True)
            weight = jnp.exp(score - top)
            top_ref[rows, head : head + 1] = top
            total_ref[rows, head : head + 1] = jnp.sum(weight, axis=1, keepdims=True)
            mixed = dot(weight.astype(BF), own_ref[seg_rows : seg_rows + keys, lanes])
            old = acc_ref[rows, lanes] if head * head_dim > lanes.start else 0.0
            acc_ref[rows, lanes] = jnp.where(mask, mixed, old)


def past_kernel(head_dim, pred_ref, *refs):
    qc_ref, pair_ref, ahead_ref, back_ref, pos_ref, top_ref, total_ref, acc_ref = refs[:8]
    out_ref, key_ref, value_ref = refs[8:]
    seg_rows, width = qc_ref.shape
    index = lax.axis_index("seg")
    present = pred_ref[0] >= 0
    behind = index - pred_ref[0]
    in_pair = behind == 2 * (index % 2) - 1
    for start in (0, seg_rows):
        part = slice(start, start + seg_rows)
        chosen = jnp.where(behind == -1, back_ref[part], ahead_ref[part])
        chosen = jnp.where(in_pair, pair_ref[part], chosen)
        if start:
            value_ref[...] = chosen
        else:
            key_ref[...] = turned(chosen)
    for block in range(seg_rows // ROWS):
        rows = slice(block * ROWS, (block + 1) * ROWS)
        out = {}
        for head, lanes, mask in head_lanes(width, head_dim):
            with_content = jnp.where(mask, qc_ref[rows, lanes], 0)
            score = dot(with_content, key_ref[lanes]) + pos_ref[head, rows]
            score = jnp.where(present, score, MASKED)
            now_top = top_ref[rows, head : head + 1]
            top = jnp.maximum(now_top, jnp.max(score, axis=1, keepdims=True))
            weight = jnp.exp(score - top)
            decay = jnp.exp(now_top - top)
            total = total_ref[rows, head : head + 1] * decay + jnp.sum(weight, axis=1, keepdims=True)
            mixed = acc_ref[rows, lanes] * decay + dot(weight.astype(BF), value_ref[:, lanes])
            mixed = mixed * (1.0 / total)
            old = out.get(lanes.start, 0.0)
            out[lanes.start] = jnp.where(mask, mixed, old)
        for start, value in out.items():
            out_ref[rows, start : start + value.shape[1]] = value.astype(BF)


def attend_now(with_content, with_position, own, rel_keys, head_dim):
    seg_rows, width = with_content.shape
    heads = width // head_dim
    stats = jax.ShapeDtypeStruct((seg_rows, 128), F32)
    return pl.pallas_call(
        lambda *refs: now_kernel(head_dim, *refs),
        out_shape=(
            jax.ShapeDtypeStruct((heads, seg_rows, seg_rows), F32),
            stats,
            stats,
            jax.ShapeDtypeStruct((seg_rows, width), F32),
        ),
        in_specs=[IN_VMEM] * 4,
        out_specs=[IN_VMEM] * 4,
        scratch_shapes=[pltpu.VMEM((width, seg_rows), BF)],
        compiler_params=room(12),
        name="attend_now",
    )(*[near(a) for a in (with_content, with_position, own, rel_keys)])


def attend_past(pred, with_content, sources, local, head_dim):
    seg_rows, width = with_content.shape
    return pl.pallas_call(
        lambda *refs: past_kernel(head_dim, *refs),
        out_shape=jax.ShapeDtypeStruct((seg_rows, width), BF),
        in_specs=[IN_SMEM] + [IN_VMEM] * 8,
        out_specs=IN_VMEM,
        scratch_shapes=[pltpu.VMEM((width, seg_rows), BF), pltpu.VMEM((seg_rows, width), BF)],
        compiler_params=room(12),
        name="attend_past",
    )(pred, *[near(a) for a in (with_content, *sources, *local)])


def fetch_first(own, behind):
    count = lax.axis_size("seg")
    onward = [(k, k + (1 if k % 2 else 3)) for k in range(count)]
    onward = [(k, j) for k, j in onward if j < count]
    pair = swapped(own, "seg", 1)
    older = lax.ppermute(own, "seg", [(k, k + 2) for k in range(1, count - 2, 2)])
    wanted = lax.ppermute(behind, "seg", [(j, k) for k, j in onward])
    return pair, older, wanted, onward


def choose_kernel(wanted_ref, facts_ref, own_ref, pair_ref, older_ref, out_ref, sem):
    odd = lax.axis_index("seg") % 2
    wanted = wanted_ref[0] + facts_ref[0]
    use_own = wanted == 3 - 2 * odd
    use_older = (odd == 1) & (wanted == 3)

    @pl.when(use_older)
    def _():
        copy = pltpu.make_async_copy(older_ref, out_ref, sem)
        copy.start()
        copy.wait()

    @pl.when(jnp.logical_not(use_older))
    def _():
        out_ref[...] = jnp.where(use_own, own_ref[...], pair_ref[...])


def fetch_second(own, pair, older, wanted, facts, onward):
    count = lax.axis_size("seg")
    passed = pl.pallas_call(
        choose_kernel,
        out_shape=jax.ShapeDtypeStruct(own.shape, BF),
        in_specs=[IN_SMEM] * 2 + [IN_VMEM] * 2 + [IN_PLACE],
        out_specs=IN_VMEM,
        scratch_shapes=[pltpu.SemaphoreType.DMA],
        compiler_params=room(8),
        name="choose",
    )(wanted, facts, near(own), near(pair), afar(older))
    ahead = lax.ppermute(passed, "seg", onward)
    back = lax.ppermute(pair, "seg", [(k, k - 2) for k in range(3, count, 2)])
    return ahead, back


def gathered(block, axis):
    distance = lax.axis_size(axis) // 2
    far = {0: block}
    while distance >= 1:
        far = {**far, **{d | distance: swapped(b, axis, distance) for d, b in far.items()}}
        distance //= 2
    return [far[d] for d in range(lax.axis_size(axis))]


def mid_kernel(parts, role, *refs):
    heads = refs[:parts]
    outs = refs[parts : 2 * parts]
    (embedded, gain, shift, w_up, up_bias, w_down, partial_ref, first_ref) = refs[2 * parts :]
    count = partial_ref.shape[0]
    half = (lax.axis_index("mp") + role) % 2
    for block in range(count // ROWS):
        rows = pl.ds(pl.multiple_of(half * count + block * ROWS, ROWS), ROWS)
        put = slice(block * ROWS, (block + 1) * ROWS)
        total = embedded[rows].astype(F32)
        for head, out in zip(heads, outs):
            total = total + dot(head[rows], out[...]).astype(BF).astype(F32)
        first = normalize(total, gain[...], shift[...]).astype(BF)
        first_ref[put] = first
        units = jnp.maximum(dot(first, w_up[...]) + up_bias[...], 0.0).astype(BF)
        partial_ref[put] = dot(units, w_down[...]).astype(BF)


def feed_forward(role, attended, outs, embedded, gain, shift, w_up, up_bias, w_down):
    seg_rows, features = embedded.shape
    parts = len(attended)
    return pl.pallas_call(
        lambda *refs: mid_kernel(parts, role, *refs),
        in_specs=[IN_VMEM] * (2 * parts + 6),
        out_specs=[IN_VMEM, IN_VMEM],
        out_shape=(jax.ShapeDtypeStruct((seg_rows // 2, features), BF),) * 2,
        compiler_params=room(16),
        name="feed_forward",
    )(*[near(a) for a in (*attended, *outs, embedded)], gain, shift, near(w_up), up_bias, near(w_down))


def second_kernel(count, *refs):
    terms = refs[:count]
    first, bias, gain, shift, out_ref = refs[count:]
    total = first[...].astype(F32) + bias[...]
    for term in terms:
        total = total + term[...].astype(F32)
    out_ref[...] = normalize(total, gain[...], shift[...]).astype(BF)


def vocab_kernel(role, rows_ref, w_ref, targets_ref, out_ref, logits_ref):
    count = rows_ref.shape[0]
    words = w_ref.shape[1]
    rows = rows_ref[...]
    index = lax.axis_index("mp")
    ids = jnp.where((index + role) % 2 == 0, targets_ref[0:1], targets_ref[1:2])
    ids = (ids - index * words).astype(F32)
    ids = jnp.broadcast_to(ids, (8, count)).T[:, :1].astype(jnp.int32)
    lanes = lax.broadcasted_iota(jnp.int32, (count, 128), 1)
    chunk = 512
    tops = None
    for start in range(0, words, chunk):
        logits = dot(rows, w_ref[:, start : start + chunk])
        logits_ref[:, start : start + chunk] = logits
        for at in range(0, chunk, 128):
            piece = logits[:, at : at + 128]
            tops = piece if tops is None else jnp.maximum(tops, piece)
    top = jnp.max(tops, axis=1, keepdims=True)
    total = jnp.zeros((count, 128), F32)
    picked = jnp.zeros((count, 128), F32)
    for start in range(0, words, 128):
        piece = logits_ref[:, start : start + 128]
        total = total + jnp.exp(piece - top)
        picked = picked + jnp.where(lanes == ids - start, piece, 0.0)
    total = jnp.sum(total, axis=1, keepdims=True)
    picked = jnp.sum(picked, axis=1, keepdims=True)
    packed = jnp.where(lanes == 0, top, jnp.where(lanes == 1, total, picked))
    out_ref[...] = packed.T[:8]


def vocab_stats(role, rows, w_vocab, targets):
    count = rows.shape[0]
    return pl.pallas_call(
        lambda *refs: vocab_kernel(role, *refs),
        in_specs=[IN_VMEM] * 3,
        out_specs=IN_VMEM,
        out_shape=jax.ShapeDtypeStruct((8, count), F32),
        scratch_shapes=[pltpu.VMEM((count, w_vocab.shape[1]), F32)],
        compiler_params=room(16),
        name="vocab_stats",
    )(near(rows), near(w_vocab), targets)


def token_kernel(facts_ref, stats_ref, token_ref, sums_ref):
    count, _, half_rows = stats_ref.shape
    valid = facts_ref[1]
    whole = jnp.zeros((1, 1), F32)
    for half in range(2):
        at = [3 * (half ^ (k & 1)) for k in range(count)]
        tops = [stats_ref[k, a : a + 1] for k, a in enumerate(at)]
        top = tops[0]
        for other in tops[1:]:
            top = jnp.maximum(top, other)
        total = sum(stats_ref[k, a + 1 : a + 2] * jnp.exp(tops[k] - top) for k, a in enumerate(at))
        picked = sum(stats_ref[k, a + 2 : a + 3] for k, a in enumerate(at))
        rows = lax.broadcasted_iota(jnp.int32, (1, half_rows), 1) + half * half_rows
        terms = jnp.where(rows < valid, picked - (top + jnp.log(total)), 0.0)
        token_ref[:, half * half_rows : (half + 1) * half_rows] = terms
        whole = whole + jnp.sum(terms, axis=1, keepdims=True)
    shape = sums_ref.shape
    row = lax.broadcasted_iota(jnp.int32, shape, 0)
    slot = lax.broadcasted_iota(jnp.int32, shape, 1)
    values = jnp.where(row == 0, jnp.broadcast_to(whole, shape), valid.astype(F32))
    sums_ref[...] = jnp.where(slot == facts_ref[2], values, 0.0)


def token_terms_of(facts, stats):
    return pl.pallas_call(
        token_kernel,
        in_specs=[IN_SMEM, IN_VMEM],
        out_specs=[IN_VMEM] * 2,
        out_shape=(
            jax.ShapeDtypeStruct((1, 2 * stats.shape[2]), F32),
            jax.ShapeDtypeStruct((8, 128), F32),
        ),
        compiler_params=room(4),
        name="token_terms",
    )(facts, near(stats))


def on_device(
    embedded,
    targets,
    pred_device,
    doc_ids,
    valid_rows,
    w_query,
    w_key,
    w_value,
    w_rel,
    content_bias,
    position_bias,
    attn_out,
    attn_gain,
    attn_shift,
    w_up,
    up_bias,
    w_down,
    down_bias,
    ffn_gain,
    ffn_shift,
    w_vocab,
):
    seg_rows, _ = embedded.shape
    head_dim = content_bias.shape[1]
    score_scale = head_dim ** (-0.5)
    row = lambda a: a.reshape(1, -1)
    behind = lax.axis_index("seg") - pred_device
    own = keys_and_values(embedded, w_key, w_value)
    pair, older, wanted, onward = fetch_first(own, behind)
    with_content, with_position, rel_keys, halves, facts = prepare(
        embedded, w_query, row(content_bias), row(position_bias), w_rel, targets, valid_rows, doc_ids, score_scale
    )
    local = attend_now(with_content, with_position, own, rel_keys, head_dim)
    ahead, back = fetch_second(own, pair, older, wanted, facts, onward)
    outs = gathered(attn_out, "mp")
    attended = attend_past(pred_device, with_content, (pair, ahead, back), local, head_dim)
    w_up, w_down = load([w_up, w_down], attended)
    attended = gathered(attended, "mp")
    mp_count = lax.axis_size("mp")
    forward = lambda role: feed_forward(
        role,
        attended,
        outs,
        embedded,
        row(attn_gain),
        row(attn_shift),
        w_up,
        row(up_bias),
        w_down,
    )
    given, _ = forward(1)
    kept, first_out = forward(0)
    (w_vocab,) = load([w_vocab], kept)
    terms = [kept, swapped(given, "mp", 1)]
    distance = 2
    while distance < mp_count:
        terms = [(terms[0].astype(F32) + terms[1].astype(F32)).astype(BF)]
        terms.append(swapped(terms[0], "mp", distance))
        distance *= 2
    second = pl.pallas_call(
        lambda *refs: second_kernel(len(terms), *refs),
        out_shape=jax.ShapeDtypeStruct(first_out.shape, BF),
        compiler_params=room(8),
        name="second",
    )(*[near(t) for t in terms], near(first_out), row(down_bias), row(ffn_gain), row(ffn_shift))
    other = swapped(second, "mp", 1)
    stats_mine = vocab_stats(0, second, w_vocab, halves)
    stats_other = vocab_stats(1, other, w_vocab, halves)
    stats = lax.all_gather(jnp.concatenate([stats_mine[:3], stats_other[:3]], axis=0), "mp")
    token_terms, sums = token_terms_of(facts, stats)
    doc_slots = lax.axis_size("seg") // DOC_SPAN
    distance = 1
    while distance < lax.axis_size("seg"):
        wide = distance > 1 and 4 * distance <= lax.axis_size("seg")
        steps = (1, 2, 3) if wide else (1,)
        sums = sum([swapped(sums, "seg", distance * step) for step in steps], sums)
        distance *= 1 + len(steps)
    return (token_terms.reshape(seg_rows), sums[0, :doc_slots] / sums[1, :doc_slots])


def solution(mesh):
    return jax.shard_map(
        on_device,
        mesh=mesh,
        in_specs=(
            P("seg", None),
            P("seg"),
            P("seg"),
            P("seg"),
            P("seg"),
            P(None, "mp"),
            P(None, "mp"),
            P(None, "mp"),
            P(None, "mp"),
            P("mp", None),
            P("mp", None),
            P("mp", None),
            P(),
            P(),
            P(None, "mp"),
            P("mp"),
            P("mp", None),
            P(),
            P(),
            P(),
            P(None, "mp"),
        ),
        out_specs=(P("seg"), P()),
        check_vma=False,
    )
```

```python
import jax
import jax.numpy as jnp
from jax import lax
from jax.experimental import pallas as pl
from jax.experimental.pallas import tpu as pltpu
from jax.sharding import PartitionSpec as P

DOC_SPAN = 4
EPSILON = 1e-05
STEP = 32
ROWS = 256
PARTS = 4
CHUNKS = 2
MASKED = -1e30
BF = jnp.bfloat16
F32 = jnp.float32


def swapped(block, axis, distance):
    return lax.ppermute(block, axis, [(i, i ^ distance) for i in range(lax.axis_size(axis))])


def dot(a, b):
    return jnp.dot(a, b, preferred_element_type=F32)


def near(a):
    return pltpu.with_memory_space_constraint(a, pltpu.MemorySpace.VMEM)


def afar(a):
    return pltpu.with_memory_space_constraint(a, pltpu.MemorySpace.HBM)


def room(mebibytes):
    return pltpu.CompilerParams(vmem_limit_bytes=mebibytes << 20)


IN_VMEM = pl.BlockSpec(memory_space=pltpu.VMEM)
IN_SMEM = pl.BlockSpec(memory_space=pltpu.SMEM)
IN_PLACE = pl.BlockSpec(memory_space=pltpu.MemorySpace.HBM)


def chunk_copies(source, target, sems, parts):
    rows = source.shape[0] // parts
    return [
        pltpu.make_async_copy(
            source.at[pl.ds(k * rows, rows)], target.at[pl.ds(k * rows, rows)], sems.at[k]
        )
        for k in range(parts)
    ]


def kv_kernel(embedded_ref, key_ref, value_ref, out_ref, rows_ref, key_near, value_near, sems):
    seg_rows = embedded_ref.shape[0]
    loads = [
        chunk_copies(source, target, sems.at[k], PARTS)
        for k, (source, target) in enumerate(
            [(key_ref, key_near), (embedded_ref, rows_ref), (value_ref, value_near)]
        )
    ]
    for copies in loads:
        for copy in copies:
            copy.start()
    for copy in loads[0]:
        copy.wait()
    half = seg_rows // 2
    for k in range(2):
        for copy in loads[1][k * PARTS // 2 : (k + 1) * PARTS // 2]:
            copy.wait()
        part = slice(k * half, (k + 1) * half)
        out_ref[part] = dot(rows_ref[part], key_near[...]).astype(BF)
    for copy in loads[2]:
        copy.wait()
    out_ref[seg_rows:] = dot(rows_ref[...], value_near[...]).astype(BF)


def keys_and_values(embedded, w_key, w_value):
    return pl.pallas_call(
        kv_kernel,
        out_shape=jax.ShapeDtypeStruct((2 * embedded.shape[0], w_key.shape[1]), BF),
        in_specs=[IN_PLACE] * 3,
        out_specs=IN_VMEM,
        scratch_shapes=[
            pltpu.VMEM(embedded.shape, BF),
            pltpu.VMEM(w_key.shape, BF),
            pltpu.VMEM(w_value.shape, BF),
            pltpu.SemaphoreType.DMA((3, PARTS)),
        ],
        compiler_params=room(12),
        name="keys_and_values",
    )(afar(embedded), afar(w_key), afar(w_value))


def load_kernel(count, *refs):
    sources, targets, sems = refs[:count], refs[count + 1 : 2 * count + 1], refs[2 * count + 1]
    copies = []
    for k, (source, target) in enumerate(zip(sources, targets)):
        copies += chunk_copies(source, target, sems.at[k], PARTS)
    for copy in copies:
        copy.start()
    for copy in copies:
        copy.wait()


def load(weights, after):
    count = len(weights)
    return pl.pallas_call(
        lambda *refs: load_kernel(count, *refs),
        out_shape=[jax.ShapeDtypeStruct(w.shape, w.dtype) for w in weights],
        in_specs=[IN_PLACE] * count + [pl.BlockSpec(memory_space=pl.ANY)],
        out_specs=[IN_VMEM] * count,
        scratch_shapes=[pltpu.SemaphoreType.DMA((count, PARTS))],
        compiler_params=room(4),
        name="load",
    )(*[afar(w) for w in weights], after)


def turned(a):
    return a.astype(F32).T.astype(BF)


def normalize(values, norm_gain, norm_shift):
    centre = values - jnp.mean(values, axis=-1, keepdims=True)
    spread = jnp.mean(centre * centre, axis=-1, keepdims=True)
    return centre * lax.rsqrt(spread + EPSILON) * norm_gain + norm_shift


def prepare_kernel(scale, *refs):
    rows_ref, query_ref, content_ref, position_ref, coarse_ref, fine_ref, weight_ref, targets_ref = refs[:8]
    valid_ref, doc_ref, qc_ref, qp_ref, out_ref, halves_ref, facts_ref = refs[8:]
    halves_ref[...] = targets_ref[...]
    facts_ref[0] = 0
    facts_ref[1] = valid_ref[0]
    facts_ref[2] = doc_ref[0]
    queries = dot(rows_ref[...], query_ref[...])
    qc_ref[...] = (queries + content_ref[...]).astype(BF) * BF(scale)
    qp_ref[...] = (queries + position_ref[...]).astype(BF) * BF(scale)
    half = coarse_ref.shape[2]
    group = 256 // STEP
    sin_fine = fine_ref[0][None]
    cos_fine = fine_ref[1][None]
    for block in range(coarse_ref.shape[1] // group):
        sin_coarse = coarse_ref[0, block * group : (block + 1) * group][:, None]
        cos_coarse = coarse_ref[1, block * group : (block + 1) * group][:, None]
        sines = (sin_coarse * cos_fine + cos_coarse * sin_fine).reshape(256, half).astype(BF)
        cosines = (cos_coarse * cos_fine - sin_coarse * sin_fine).reshape(256, half).astype(BF)
        rel = dot(sines, weight_ref[:half]) + dot(cosines, weight_ref[half:])
        out_ref[:, block * 256 : (block + 1) * 256] = rel.T.astype(BF)


def prepare(embedded, w_query, content_bias, position_bias, w_rel, targets, valid_rows, doc_ids, scale):
    seg_rows, features = embedded.shape
    length = 2 * seg_rows
    width = w_query.shape[1]
    frequency = 10000.0 ** (-jnp.arange(0, features, 2).astype(F32) / features)
    coarse = (jnp.arange(length // STEP)[::-1] * STEP).astype(F32)[:, None] * frequency[None]
    fine = jnp.arange(STEP)[::-1].astype(F32)[:, None] * frequency[None]
    queries = jax.ShapeDtypeStruct((seg_rows, width), BF)
    return pl.pallas_call(
        lambda *refs: prepare_kernel(scale, *refs),
        out_shape=(
            queries,
            queries,
            jax.ShapeDtypeStruct((width, length), BF),
            jax.ShapeDtypeStruct((2, seg_rows // 2), jnp.int32),
            jax.ShapeDtypeStruct((3,), jnp.int32),
        ),
        in_specs=[IN_VMEM] * 8 + [IN_SMEM] * 2,
        out_specs=[IN_VMEM] * 4 + [IN_SMEM],
        compiler_params=room(12),
        name="prepare",
    )(
        near(embedded),
        near(w_query),
        content_bias,
        position_bias,
        near(jnp.stack([jnp.sin(coarse), jnp.cos(coarse)])),
        near(jnp.stack([jnp.sin(fine), jnp.cos(fine)])),
        near(w_rel),
        targets.reshape(2, seg_rows // 2),
        valid_rows,
        doc_ids,
    )


def head_lanes(width, head_dim):
    lanes = min(width, max(128, head_dim))
    at = lax.broadcasted_iota(jnp.int32, (1, lanes), 1)
    for head in range(width // head_dim):
        start = head * head_dim // lanes * lanes
        first = head * head_dim - start
        yield head, slice(start, start + lanes), (at >= first) & (at < first + head_dim)


def now_kernel(head_dim, *refs):
    qc_ref, qp_ref, own_ref, rel_ref, pos_ref, top_ref, total_ref, acc_ref, key_ref = refs
    seg_rows, width = qc_ref.shape
    span = rel_ref.shape[1]
    key_ref[...] = turned(own_ref[:seg_rows])
    for block in range(seg_rows // ROWS):
        first = block * ROWS
        rows = slice(first, first + ROWS)
        keys = first + ROWS
        columns = lax.broadcasted_iota(jnp.int32, (ROWS, keys), 1)
        causal = columns <= lax.broadcasted_iota(jnp.int32, (ROWS, keys), 0) + first
        for head, lanes, mask in head_lanes(width, head_dim):
            with_content = jnp.where(mask, qc_ref[rows, lanes], 0)
            with_position = jnp.where(mask, qp_ref[rows, lanes], 0)
            skewed = dot(with_position, rel_ref[lanes])
            position = pltpu.roll(skewed, (seg_rows + 1 + first) % span, 1, stride=1, stride_axis=0)
            pos_ref[head, rows] = position[:, :seg_rows]
            score = dot(with_content, key_ref[lanes, :keys]) + position[:, seg_rows : seg_rows + keys]
            score = jnp.where(causal, score, MASKED)
            top = jnp.max(score, axis=1, keepdims=True)
            weight = jnp.exp(score - top)
            top_ref[rows, head : head + 1] = top
            total_ref[rows, head : head + 1] = jnp.sum(weight, axis=1, keepdims=True)
            mixed = dot(weight.astype(BF), own_ref[seg_rows : seg_rows + keys, lanes])
            old = acc_ref[rows, lanes] if head * head_dim > lanes.start else 0.0
            acc_ref[rows, lanes] = jnp.where(mask, mixed, old)


def past_kernel(head_dim, pred_ref, *refs):
    qc_ref, pair_ref, ahead_ref, back_ref, pos_ref, top_ref, total_ref, acc_ref = refs[:8]
    out_ref, key_ref, value_ref = refs[8:]
    seg_rows, width = qc_ref.shape
    index = lax.axis_index("seg")
    present = pred_ref[0] >= 0
    behind = index - pred_ref[0]
    in_pair = behind == 2 * (index % 2) - 1
    for start in (0, seg_rows):
        part = slice(start, start + seg_rows)
        chosen = jnp.where(behind == -1, back_ref[part], ahead_ref[part])
        chosen = jnp.where(in_pair, pair_ref[part], chosen)
        if start:
            value_ref[...] = chosen
        else:
            key_ref[...] = turned(chosen)
    for block in range(seg_rows // ROWS):
        rows = slice(block * ROWS, (block + 1) * ROWS)
        out = {}
        for head, lanes, mask in head_lanes(width, head_dim):
            with_content = jnp.where(mask, qc_ref[rows, lanes], 0)
            score = dot(with_content, key_ref[lanes]) + pos_ref[head, rows]
            score = jnp.where(present, score, MASKED)
            now_top = top_ref[rows, head : head + 1]
            top = jnp.maximum(now_top, jnp.max(score, axis=1, keepdims=True))
            weight = jnp.exp(score - top)
            decay = jnp.exp(now_top - top)
            total = total_ref[rows, head : head + 1] * decay + jnp.sum(weight, axis=1, keepdims=True)
            mixed = acc_ref[rows, lanes] * decay + dot(weight.astype(BF), value_ref[:, lanes])
            mixed = mixed * (1.0 / total)
            old = out.get(lanes.start, 0.0)
            out[lanes.start] = jnp.where(mask, mixed, old)
        for start, value in out.items():
            out_ref[rows, start : start + value.shape[1]] = value.astype(BF)


def attend_now(with_content, with_position, own, rel_keys, head_dim):
    seg_rows, width = with_content.shape
    heads = width // head_dim
    stats = jax.ShapeDtypeStruct((seg_rows, 128), F32)
    return pl.pallas_call(
        lambda *refs: now_kernel(head_dim, *refs),
        out_shape=(
            jax.ShapeDtypeStruct((heads, seg_rows, seg_rows), F32),
            stats,
            stats,
            jax.ShapeDtypeStruct((seg_rows, width), F32),
        ),
        in_specs=[IN_VMEM] * 4,
        out_specs=[IN_VMEM] * 4,
        scratch_shapes=[pltpu.VMEM((width, seg_rows), BF)],
        compiler_params=room(12),
        name="attend_now",
    )(*[near(a) for a in (with_content, with_position, own, rel_keys)])


def attend_past(pred, with_content, sources, local, head_dim):
    seg_rows, width = with_content.shape
    return pl.pallas_call(
        lambda *refs: past_kernel(head_dim, *refs),
        out_shape=jax.ShapeDtypeStruct((seg_rows, width), BF),
        in_specs=[IN_SMEM] + [IN_VMEM] * 8,
        out_specs=IN_VMEM,
        scratch_shapes=[pltpu.VMEM((width, seg_rows), BF), pltpu.VMEM((seg_rows, width), BF)],
        compiler_params=room(12),
        name="attend_past",
    )(pred, *[near(a) for a in (with_content, *sources, *local)])


def fetch_first(own, behind):
    count = lax.axis_size("seg")
    onward = [(k, k + (1 if k % 2 else 3)) for k in range(count)]
    onward = [(k, j) for k, j in onward if j < count]
    pair = swapped(own, "seg", 1)
    older = lax.ppermute(own, "seg", [(k, k + 2) for k in range(1, count - 2, 2)])
    wanted = lax.ppermute(behind, "seg", [(j, k) for k, j in onward])
    return pair, older, wanted, onward


def choose_kernel(wanted_ref, facts_ref, own_ref, pair_ref, older_ref, out_ref, sem):
    odd = lax.axis_index("seg") % 2
    wanted = wanted_ref[0] + facts_ref[0]
    use_own = wanted == 3 - 2 * odd
    use_older = (odd == 1) & (wanted == 3)

    @pl.when(use_older)
    def _():
        copy = pltpu.make_async_copy(older_ref, out_ref, sem)
        copy.start()
        copy.wait()

    @pl.when(jnp.logical_not(use_older))
    def _():
        out_ref[...] = jnp.where(use_own, own_ref[...], pair_ref[...])


def fetch_second(own, pair, older, wanted, facts, onward):
    count = lax.axis_size("seg")
    passed = pl.pallas_call(
        choose_kernel,
        out_shape=jax.ShapeDtypeStruct(own.shape, BF),
        in_specs=[IN_SMEM] * 2 + [IN_VMEM] * 2 + [IN_PLACE],
        out_specs=IN_VMEM,
        scratch_shapes=[pltpu.SemaphoreType.DMA],
        compiler_params=room(8),
        name="choose",
    )(wanted, facts, near(own), near(pair), afar(older))
    ahead = lax.ppermute(passed, "seg", onward)
    back = lax.ppermute(pair, "seg", [(k, k - 2) for k in range(3, count, 2)])
    return ahead, back


def gathered(block, axis):
    distance = lax.axis_size(axis) // 2
    far = {0: block}
    while distance >= 1:
        far = {**far, **{d | distance: swapped(b, axis, distance) for d, b in far.items()}}
        distance //= 2
    return [far[d] for d in range(lax.axis_size(axis))]


def mid_kernel(parts, chunk, *refs):
    heads = refs[:parts]
    outs = refs[parts : 2 * parts]
    embedded, gain, shift, w_up, up_bias, w_down, given_ref, kept_ref, first_ref = refs[2 * parts :]
    count = given_ref.shape[0]
    half_rows = embedded.shape[0] // 2
    mine = lax.axis_index("mp") % 2
    starts = [pl.multiple_of(h * half_rows + chunk * count, count) for h in (1 - mine, mine)]
    rows_of = lambda ref: jnp.concatenate([ref[pl.ds(start, count)] for start in starts], axis=0)
    total = rows_of(embedded).astype(F32)
    for head, out in zip(heads, outs):
        total = total + dot(rows_of(head), out[...]).astype(BF).astype(F32)
    first = normalize(total, gain[...], shift[...]).astype(BF)
    first_ref[...] = first[count:]
    units = jnp.maximum(dot(first, w_up[...]) + up_bias[...], 0.0).astype(BF)
    partial = dot(units, w_down[...]).astype(BF)
    given_ref[...] = partial[:count]
    kept_ref[...] = partial[count:]


def feed_forward(chunk, attended, outs, embedded, gain, shift, w_up, up_bias, w_down):
    seg_rows, features = embedded.shape
    parts = len(attended)
    return pl.pallas_call(
        lambda *refs: mid_kernel(parts, chunk, *refs),
        in_specs=[IN_VMEM] * (2 * parts + 6),
        out_specs=[IN_VMEM] * 3,
        out_shape=(jax.ShapeDtypeStruct((seg_rows // 2 // CHUNKS, features), BF),) * 3,
        compiler_params=room(16),
        name="feed_forward",
    )(*[near(a) for a in (*attended, *outs, embedded)], gain, shift, near(w_up), up_bias, near(w_down))


def second_kernel(count, *refs):
    terms = refs[:count]
    first, bias, gain, shift, out_ref = refs[count:]
    total = first[...].astype(F32) + bias[...]
    for term in terms:
        total = total + term[...].astype(F32)
    out_ref[...] = normalize(total, gain[...], shift[...]).astype(BF)


def vocab_kernel(chunk, mine_ref, other_ref, w_ref, targets_ref, out_ref, logits_ref):
    piece_rows = mine_ref.shape[0]
    count = 2 * piece_rows
    words = w_ref.shape[1]
    rows = jnp.concatenate([mine_ref[...], other_ref[...]], axis=0)
    index = lax.axis_index("mp")
    piece = slice(chunk * piece_rows, (chunk + 1) * piece_rows)
    low, high = targets_ref[0:1, piece], targets_ref[1:2, piece]
    ids = jnp.concatenate(
        [jnp.where(index % 2 == 0, low, high), jnp.where(index % 2 == 0, high, low)], axis=1
    )
    ids = (ids - index * words).astype(F32)
    ids = jnp.broadcast_to(ids, (8, count)).T[:, :1].astype(jnp.int32)
    lanes = lax.broadcasted_iota(jnp.int32, (count, 128), 1)
    chunk = 512
    tops = None
    for start in range(0, words, chunk):
        logits = dot(rows, w_ref[:, start : start + chunk])
        logits_ref[:, start : start + chunk] = logits
        for at in range(0, chunk, 128):
            piece = logits[:, at : at + 128]
            tops = piece if tops is None else jnp.maximum(tops, piece)
    top = jnp.max(tops, axis=1, keepdims=True)
    total = jnp.zeros((count, 128), F32)
    picked = jnp.zeros((count, 128), F32)
    for start in range(0, words, 128):
        piece = logits_ref[:, start : start + 128]
        total = total + jnp.exp(piece - top)
        picked = picked + jnp.where(lanes == ids - start, piece, 0.0)
    total = jnp.sum(total, axis=1, keepdims=True)
    picked = jnp.sum(picked, axis=1, keepdims=True)
    packed = jnp.where(lanes == 0, top, jnp.where(lanes == 1, total, picked))
    out_ref[...] = packed.T[:8]


def vocab_stats(chunk, mine, other, w_vocab, targets):
    count = 2 * mine.shape[0]
    return pl.pallas_call(
        lambda *refs: vocab_kernel(chunk, *refs),
        in_specs=[IN_VMEM] * 4,
        out_specs=IN_VMEM,
        out_shape=jax.ShapeDtypeStruct((8, count), F32),
        scratch_shapes=[pltpu.VMEM((count, w_vocab.shape[1]), F32)],
        compiler_params=room(16),
        name="vocab_stats",
    )(near(mine), near(other), near(w_vocab), targets)


def token_kernel(facts_ref, stats_ref, token_ref, sums_ref):
    count, _, width = stats_ref.shape
    piece = width // 2
    valid = facts_ref[1]
    whole = jnp.zeros((1, 1), F32)
    for block in range(2 * CHUNKS):
        half, chunk = divmod(block, CHUNKS)
        part = lambda k, row: stats_ref[
            k, 3 * chunk + row : 3 * chunk + row + 1, (half ^ (k & 1)) * piece : ((half ^ (k & 1)) + 1) * piece
        ]
        tops = [part(k, 0) for k in range(count)]
        top = tops[0]
        for other in tops[1:]:
            top = jnp.maximum(top, other)
        total = sum(part(k, 1) * jnp.exp(tops[k] - top) for k in range(count))
        picked = sum(part(k, 2) for k in range(count))
        rows = lax.broadcasted_iota(jnp.int32, (1, piece), 1) + block * piece
        terms = jnp.where(rows < valid, picked - (top + jnp.log(total)), 0.0)
        token_ref[:, block * piece : (block + 1) * piece] = terms
        whole = whole + jnp.sum(terms, axis=1, keepdims=True)
    shape = sums_ref.shape
    row = lax.broadcasted_iota(jnp.int32, shape, 0)
    slot = lax.broadcasted_iota(jnp.int32, shape, 1)
    values = jnp.where(row == 0, jnp.broadcast_to(whole, shape), valid.astype(F32))
    sums_ref[...] = jnp.where(slot == facts_ref[2], values, 0.0)


def token_terms_of(facts, stats):
    return pl.pallas_call(
        token_kernel,
        in_specs=[IN_SMEM, IN_VMEM],
        out_specs=[IN_VMEM] * 2,
        out_shape=(
            jax.ShapeDtypeStruct((1, CHUNKS * stats.shape[2]), F32),
            jax.ShapeDtypeStruct((8, 128), F32),
        ),
        compiler_params=room(4),
        name="token_terms",
    )(facts, near(stats))


def on_device(
    embedded,
    targets,
    pred_device,
    doc_ids,
    valid_rows,
    w_query,
    w_key,
    w_value,
    w_rel,
    content_bias,
    position_bias,
    attn_out,
    attn_gain,
    attn_shift,
    w_up,
    up_bias,
    w_down,
    down_bias,
    ffn_gain,
    ffn_shift,
    w_vocab,
):
    seg_rows, _ = embedded.shape
    head_dim = content_bias.shape[1]
    score_scale = head_dim ** (-0.5)
    row = lambda a: a.reshape(1, -1)
    behind = lax.axis_index("seg") - pred_device
    own = keys_and_values(embedded, w_key, w_value)
    pair, older, wanted, onward = fetch_first(own, behind)
    with_content, with_position, rel_keys, halves, facts = prepare(
        embedded, w_query, row(content_bias), row(position_bias), w_rel, targets, valid_rows, doc_ids, score_scale
    )
    local = attend_now(with_content, with_position, own, rel_keys, head_dim)
    ahead, back = fetch_second(own, pair, older, wanted, facts, onward)
    outs = gathered(attn_out, "mp")
    attended = attend_past(pred_device, with_content, (pair, ahead, back), local, head_dim)
    w_up, w_down, w_vocab = load([w_up, w_down, w_vocab], attended)
    attended = gathered(attended, "mp")
    mp_count = lax.axis_size("mp")
    terms, firsts = [], []
    for chunk in range(CHUNKS):
        given, kept, first_out = feed_forward(
            chunk,
            attended,
            outs,
            embedded,
            row(attn_gain),
            row(attn_shift),
            w_up,
            row(up_bias),
            w_down,
        )
        parts = [kept, swapped(given, "mp", 1)]
        distance = 2
        while distance < mp_count:
            parts = [(parts[0].astype(F32) + parts[1].astype(F32)).astype(BF)]
            parts.append(swapped(parts[0], "mp", distance))
            distance *= 2
        terms.append(parts)
        firsts.append(first_out)
    stats = []
    for chunk in range(CHUNKS):
        parts = terms[chunk]
        count = len(parts)
        second = pl.pallas_call(
            lambda *refs: second_kernel(count, *refs),
            out_shape=jax.ShapeDtypeStruct(firsts[chunk].shape, BF),
            compiler_params=room(8),
            name="second",
        )(*[near(t) for t in parts], near(firsts[chunk]), row(down_bias), row(ffn_gain), row(ffn_shift))
        other = swapped(second, "mp", 1)
        stats.append(vocab_stats(chunk, second, other, w_vocab, halves))
    stats = lax.all_gather(jnp.concatenate([s[:3] for s in stats], axis=0), "mp")
    token_terms, sums = token_terms_of(facts, stats)
    doc_slots = lax.axis_size("seg") // DOC_SPAN
    distance = 1
    while distance < lax.axis_size("seg"):
        wide = distance > 1 and 4 * distance <= lax.axis_size("seg")
        steps = (1, 2, 3) if wide else (1,)
        sums = sum([swapped(sums, "seg", distance * step) for step in steps], sums)
        distance *= 1 + len(steps)
    return (token_terms.reshape(seg_rows), sums[0, :doc_slots] / sums[1, :doc_slots])


def solution(mesh):
    return jax.shard_map(
        on_device,
        mesh=mesh,
        in_specs=(
            P("seg", None),
            P("seg"),
            P("seg"),
            P("seg"),
            P("seg"),
            P(None, "mp"),
            P(None, "mp"),
            P(None, "mp"),
            P(None, "mp"),
            P("mp", None),
            P("mp", None),
            P("mp", None),
            P(),
            P(),
            P(None, "mp"),
            P("mp"),
            P("mp", None),
            P(),
            P(),
            P(),
            P(None, "mp"),
        ),
        out_specs=(P("seg"), P()),
        check_vma=False,
    )
```
